8 devices in a mesh: data: 2 (over z, y), dap: 4 (over x, core).
Axes of the slice: x: 2, y: 2, z: 1, core: 2. Of those that a mesh axis runs over, the one named last changes fastest.
Arguments:
- pair_act: bfloat16 [768, 384, 128], P(('data', 'dap')), parts along dimension 0
- pair_mask: int32 [768, 384], P(('data', 'dap')), parts along dimension 0
- d_pair_out: bfloat16 [768, 384, 128], P(('data', 'dap')), parts along dimension 0
- ln_pair: bfloat16 [2, 2, 128], replicated
- w_proj: bfloat16 [2, 128, 512], replicated
- w_gate: bfloat16 [2, 128, 128], replicated
- ln_chan: bfloat16 [2, 2, 128], replicated
- w_out: bfloat16 [2, 128, 128], replicated
Outputs:
- output 1: bfloat16 [768, 384, 128], P(('data', 'dap')), parts along dimension 0
- output 2: bfloat16 [768, 384, 128], P(('data', 'dap')), parts along dimension 0
- output 3: bfloat16 [4, 2, 128], P('data'), parts along dimension 0
- output 4: bfloat16 [4, 128, 512], P('data'), parts along dimension 0
- output 5: bfloat16 [4, 128, 128], P('data'), parts along dimension 0
- output 6: bfloat16 [4, 2, 128], P('data'), parts along dimension 0
- output 7: bfloat16 [4, 128, 128], P('data'), parts along dimension 0
There are 2 independent parts. The reference program is written for one: setup_inputs(seed, part) draws one part's arguments, and reference() takes and returns one part's arrays. A program takes and returns all parts, laid end to end along the dimension named above; an argument that names none is the same for every part.
All inputs are finite; a program needn't handle non-finite values.
Results may differ from the reference program's by a relative error of at most 0.0142309.
Values are sent between devices in bfloat16 or wider.
A program may use at most 1 GiB of HBM per device.

```python
import jax
import jax.numpy as jnp
from jax import lax

N = 384
CZ = 128
CH = 128
LN_EPS = 1e-5


def layer_norm(values, gain_vec, shift_vec, norm_axis):
    mean_val = jnp.mean(values, axis=norm_axis, keepdims=True)
    centered = values - mean_val
    variance = jnp.mean(centered * centered, axis=norm_axis, keepdims=True)
    return centered * lax.rsqrt(variance + LN_EPS) * gain_vec + shift_vec


def draw_mask(mask_key):
    key_row, key_col, key_rhole, key_chole = jax.random.split(mask_key, 4)
    row_keep = jax.random.randint(key_row, (N,), 0, 25) != 0
    col_keep = jax.random.randint(key_col, (N,), 0, 25) != 0
    row_index = jnp.arange(N)
    row_keep = row_keep & (row_index != jax.random.randint(key_rhole, (), 0, N))
    col_keep = col_keep & (row_index != jax.random.randint(key_chole, (), 0, N))
    return (row_keep[:, None] & col_keep[None, :]).astype(jnp.int32)


def setup_inputs(seed: int = 0, part: int = 0) -> dict:
    part_key = jax.random.fold_in(jax.random.key(seed), part)
    key_act, key_grad, key_mask = jax.random.split(part_key, 3)
    shared = jax.random.split(jax.random.key(seed + 1), 7)
    pair_act = jax.random.normal(key_act, (N, N, CZ), jnp.float32).astype(jnp.bfloat16)
    d_pair_out = jax.random.normal(key_grad, (N, N, CZ), jnp.float32).astype(jnp.bfloat16)
    pair_mask = draw_mask(key_mask)
    ln_pair = jnp.stack([1.0 + 0.3 * jax.random.normal(shared[0], (2, CZ), jnp.float32), 0.3 * jax.random.normal(shared[1], (2, CZ), jnp.float32)], axis=1).astype(jnp.bfloat16)
    w_proj = (jax.random.normal(shared[2], (2, CZ, 4 * CH), jnp.float32) * CZ ** -0.5).astype(jnp.bfloat16)
    w_gate = (jax.random.normal(shared[3], (2, CZ, CZ), jnp.float32) * CZ ** -0.5).astype(jnp.bfloat16)
    ln_chan = jnp.stack([1.0 + 0.3 * jax.random.normal(shared[4], (2, CH), jnp.float32), 0.3 * jax.random.normal(shared[5], (2, CH), jnp.float32)], axis=1).astype(jnp.bfloat16)
    w_out = (jax.random.normal(shared[6], (2, CH, CZ), jnp.float32) * CH ** -0.5).astype(jnp.bfloat16)
    return {'pair_act': pair_act, 'pair_mask': pair_mask, 'd_pair_out': d_pair_out, 'ln_pair': ln_pair, 'w_proj': w_proj, 'w_gate': w_gate, 'ln_chan': ln_chan, 'w_out': w_out}


def project_rows(z_rows, mask_rows, ln_p, w_proj, w_gate):
    x_norm = layer_norm(z_rows, ln_p[0], ln_p[1], -1).astype(jnp.bfloat16).astype(jnp.float32)
    proj_all = jnp.einsum('ijd,de->eij', x_norm, w_proj)
    gate_val = jax.nn.sigmoid(jnp.einsum('ijd,de->ije', x_norm, w_gate))
    lin_a, pre_ga, lin_b, pre_gb = jnp.split(proj_all, 4, axis=0)
    mask_f = mask_rows.astype(jnp.float32)
    left_proj = (mask_f * jax.nn.sigmoid(pre_ga) * lin_a).astype(jnp.bfloat16)
    right_proj = (mask_f * jax.nn.sigmoid(pre_gb) * lin_b).astype(jnp.bfloat16)
    return left_proj, right_proj, gate_val


def tri_outgoing(left_grp, right_grp):
    return jnp.einsum('cik,cjk->cij', left_grp.astype(jnp.float32), right_grp.astype(jnp.float32)).astype(jnp.bfloat16)


def tri_incoming(left_grp, right_grp):
    return jnp.einsum('cki,ckj->cij', left_grp.astype(jnp.float32), right_grp.astype(jnp.float32)).astype(jnp.bfloat16)


def finish_rows(z_rows, t_rows, gate_val, ln_q, w_out):
    y_norm = layer_norm(t_rows.astype(jnp.float32), ln_q[0][:, None, None], ln_q[1][:, None, None], 0).astype(jnp.bfloat16).astype(jnp.float32)
    update_f = jnp.einsum('cij,cd->ijd', y_norm, w_out)
    return (z_rows + gate_val * update_f).astype(jnp.bfloat16)


def tri_update(z_pair, pair_mask, ln_p, w_proj, w_gate, ln_q, w_out, incoming):
    z_blocks = z_pair.astype(jnp.float32).reshape(N // 8, 8, N, CZ)
    mask_blocks = pair_mask.reshape(N // 8, 8, N)
    prep_fn = jax.checkpoint(project_rows)
    left_blk, right_blk, gate_blk = lax.map(lambda block_in: prep_fn(block_in[0], block_in[1], ln_p, w_proj, w_gate), (z_blocks, mask_blocks))
    left_groups = jnp.swapaxes(left_blk, 0, 1).reshape(8, CH // 8, N, N)
    right_groups = jnp.swapaxes(right_blk, 0, 1).reshape(8, CH // 8, N, N)
    tri_fn = jax.checkpoint(tri_incoming if incoming else tri_outgoing)
    t_groups = lax.map(lambda block_in: tri_fn(block_in[0], block_in[1]), (left_groups, right_groups))
    t_blocks = jnp.swapaxes(t_groups.reshape(CH, N // 8, 8, N), 0, 1)
    post_fn = jax.checkpoint(finish_rows)
    out_blocks = lax.map(lambda block_in: post_fn(block_in[0], block_in[1], block_in[2], ln_q, w_out), (z_blocks, t_blocks, gate_blk))
    return out_blocks.reshape(N, N, CZ)


def reference(pair_act, pair_mask, d_pair_out, ln_pair, w_proj, w_gate, ln_chan, w_out):
    def forward(z_in, ln_pair_in, w_proj_in, w_gate_in, ln_chan_in, w_out_in):
        ln_pf = ln_pair_in.astype(jnp.float32)
        proj_f = w_proj_in.astype(jnp.float32)
        gate_f = w_gate_in.astype(jnp.float32)
        ln_qf = ln_chan_in.astype(jnp.float32)
        out_f = w_out_in.astype(jnp.float32)
        z_mid = tri_update(z_in, pair_mask, ln_pf[0], proj_f[0], gate_f[0], ln_qf[0], out_f[0], False)
        return tri_update(z_mid, pair_mask, ln_pf[1], proj_f[1], gate_f[1], ln_qf[1], out_f[1], True)
    pair_out, pull_back = jax.vjp(forward, pair_act, ln_pair, w_proj, w_gate, ln_chan, w_out)
    d_pair, d_ln_p, d_w_p, d_w_g, d_ln_q, d_w_o = pull_back(d_pair_out)
    return pair_out, d_pair, d_ln_p, d_w_p, d_w_g, d_ln_q, d_w_o
```

```python
import functools
import jax
import jax.numpy as jnp
from jax import lax
from jax.experimental import pallas as pl
from jax.experimental.pallas import tpu as pltpu
from jax.sharding import PartitionSpec as P

LN_EPS = 1e-5
AX = 'dap'
N = 384
C = 128
TI = 16
RB = 96
CB = 8
F32 = jnp.float32
BF16 = jnp.bfloat16
ICI_SWAP = [(0, 2), (2, 0), (1, 3), (3, 1)]
D2D_SWAP = [(0, 1), (1, 0), (2, 3), (3, 2)]
OWN, CROSS, PART, DIAG = 0, 2, 1, 3


def sig(v):
    return 0.5 * jnp.tanh(0.5 * v) + 0.5


def dot(a, b, ca, cb):
    return lax.dot_general(a, b, (((ca,), (cb,)), ((), ())), preferred_element_type=F32)


def hat_lanes(zr):
    mean = jnp.sum(zr, axis=-1, keepdims=True) * (1.0 / C)
    cen = zr - mean
    var = jnp.sum(cen * cen, axis=-1, keepdims=True) * (1.0 / C)
    rstd = lax.rsqrt(var + LN_EPS)
    return cen * rstd, rstd


def hat_rows(tr):
    mean = jnp.sum(tr, axis=0, keepdims=True) * (1.0 / C)
    cen = tr - mean
    var = jnp.sum(cen * cen, axis=0, keepdims=True) * (1.0 / C)
    rstd = lax.rsqrt(var + LN_EPS)
    return cen * rstd, rstd


def norm_x(zr, lnp_ref):
    xh, rstd = hat_lanes(zr)
    x = (xh * lnp_ref[0:1, :] + lnp_ref[1:2, :]).astype(BF16)
    return x, xh, rstd


def put_row(scr, i, val):
    for l in range(N // 128):
        scr[l, pl.ds(i, C, stride=TI), :] = val[:, l * 128:(l + 1) * 128]


def get_row(scr, i):
    return jnp.concatenate([scr[l, pl.ds(i, C, stride=TI), :] for l in range(N // 128)], axis=1)


def flush(scr, out_ref):
    for l in range(N // 128):
        out_ref[:, :, l * 128:(l + 1) * 128] = scr[l].reshape(C, TI, 128).astype(BF16)


def fill(scr, in_ref):
    for l in range(N // 128):
        scr[l] = in_ref[:, :, l * 128:(l + 1) * 128].astype(F32).reshape(C * TI, 128)


SCR = lambda: pltpu.VMEM((N // 128, C * TI, 128), F32)


def const_spec(shape):
    nd = len(shape)
    return pl.BlockSpec(shape, lambda *_: (0,) * nd)


def rows_spec(off=0):
    return pl.BlockSpec((TI, N, C), lambda i, *_: (i + off, 0, 0))


def chan_spec():
    return pl.BlockSpec((C, TI, N), lambda i, *_: (0, i, 0))


def cost(flops, nbytes, trans=0):
    return pl.CostEstimate(flops=int(flops), bytes_accessed=int(nbytes), transcendentals=int(trans))


def prep_body(base, z_ref, m_ref, lnp_ref, wt_ref, *rest):
    a_out, b_out, sa, sb = rest[-4:]

    def row(i, carry):
        zr = z_ref[i].astype(F32)
        x, _, _ = norm_x(zr, lnp_ref)
        mrow = m_ref[pl.ds(i, 1), :]
        p = dot(wt_ref[...], x, 1, 1)
        put_row(sa, i, mrow * sig(p[C:2 * C]) * p[0:C])
        put_row(sb, i, mrow * sig(p[3 * C:4 * C]) * p[2 * C:3 * C])
        return carry

    lax.fori_loop(0, TI, row, 0)
    flush(sa, a_out)
    flush(sb, b_out)


def prep(base, z, mask, lnp, wt, full=None):
    rows = z.shape[0]
    out = jax.ShapeDtypeStruct((C, N, N), BF16)
    spec = pl.BlockSpec((C, TI, N), lambda i, b: (0, b[0] + i, 0))
    extra = () if full is None else tuple(full)
    grid_spec = pltpu.PrefetchScalarGridSpec(
        num_scalar_prefetch=1, grid=(rows // TI,),
        in_specs=[rows_spec(), pl.BlockSpec((TI, N), lambda i, b: (i, 0)), const_spec((2, C)), const_spec((4 * C, C))]
        + [pl.BlockSpec(memory_space=pl.ANY)] * len(extra),
        out_specs=[spec, spec], scratch_shapes=[SCR(), SCR()])
    n = rows * N
    return pl.pallas_call(
        prep_body, grid_spec=grid_spec, out_shape=[out, out],
        input_output_aliases={5: 0, 6: 1} if extra else {},
        cost_estimate=cost(n * C * 4 * C * 2, n * C * 6, n * C * 2), name="prep",
    )(base, z, mask, lnp, wt, *extra)


def tri_out_body(idx, ao, ac, b, to, tc):
    for c in range(CB):
        lhs = jnp.concatenate([ao[c], ac[c]], axis=0)
        r = dot(lhs, b[c], 1, 1).astype(BF16)
        to[c] = r[:RB]
        tc[c] = r[RB:]


def row_block(k):
    return pl.BlockSpec((CB, RB, N), lambda c, idx: (c, idx[k], 0))


def part_block():
    return pl.BlockSpec((CB, RB, N), lambda c, idx: (c, 0, 0))


def full_block():
    return pl.BlockSpec((CB, N, N), lambda c, idx: (c, 0, 0))


PART_SHAPE = jax.ShapeDtypeStruct((C, RB, N), BF16)


def tri_call(body, idx, ins, specs, n_out, scratch, flops, name):
    grid_spec = pltpu.PrefetchScalarGridSpec(
        num_scalar_prefetch=1, grid=(C // CB,), in_specs=specs,
        out_specs=[part_block()] * n_out, scratch_shapes=scratch)
    return pl.pallas_call(body, grid_spec=grid_spec, out_shape=[PART_SHAPE] * n_out,
                          cost_estimate=cost(flops, 100e6), name=name)(idx, *ins)


def tri_out(idx, a, b):
    return tri_call(tri_out_body, idx, (a, a, b), [row_block(0), row_block(1), full_block()], 2, [], 2 * RB * N * N * C * 2, "tri_out")


def tri_in_body(idx, a, b, to, tc, s):
    ro = pl.multiple_of(idx[0] * RB, RB)
    rc = pl.multiple_of(idx[1] * RB, RB)
    for c in range(CB):
        s[c] = a[c].T
        lhs = jnp.concatenate([s[c, pl.ds(ro, RB), :], s[c, pl.ds(rc, RB), :]], axis=0)
        r = dot(lhs, b[c], 1, 0).astype(BF16)
        to[c] = r[:RB]
        tc[c] = r[RB:]


def tri_in(idx, a, b):
    return tri_call(tri_in_body, idx, (a, b), [full_block(), full_block()], 2, [pltpu.VMEM((CB, N, N), BF16)], 2 * RB * N * N * C * 2, "tri_in")


def gather_dt(idx, parts, c, s):
    for k, part in enumerate(parts):
        s[c, pl.ds(pl.multiple_of(idx[k] * RB, RB), RB), :] = part[c]


def tri_in_bwd_body(idx, d0, d1, d2, d3, ao, ac, bo, bc, dao, dac, dbo, dbc, s):
    for c in range(CB):
        gather_dt(idx, (d0, d1, d2, d3), c, s)
        da = dot(jnp.concatenate([bo[c], bc[c]], axis=0), s[c], 1, 1).astype(BF16)
        db = dot(jnp.concatenate([ao[c], ac[c]], axis=0), s[c], 1, 0).astype(BF16)
        dao[c] = da[:RB]
        dac[c] = da[RB:]
        dbo[c] = db[:RB]
        dbc[c] = db[RB:]


def tri_in_bwd(idx, dts, a, b):
    return tri_call(tri_in_bwd_body, idx, (*dts, a, a, b, b),
                    [part_block()] * 4 + [row_block(0), row_block(1)] * 2, 4, [pltpu.VMEM((CB, N, N), BF16)], 4 * RB * N * N * C * 2, "tri_in_bwd")


def tri_out_bwd_body(idx, d0, d1, d2, d3, a, b, da, db, s, st):
    ro = pl.multiple_of(idx[0] * RB, RB)
    for c in range(CB):
        gather_dt(idx, (d0, d1, d2, d3), c, s)
        da[c] = dot(d0[c], b[c], 1, 0).astype(BF16)
        st[c] = s[c].T
        db[c] = dot(st[c, pl.ds(ro, RB), :], a[c], 1, 0).astype(BF16)


def tri_out_bwd(idx, dts, a, b):
    return tri_call(tri_out_bwd_body, idx, (*dts, a, b), [part_block()] * 4 + [full_block()] * 2, 2,
                    [pltpu.VMEM((CB, N, N), BF16), pltpu.VMEM((CB, N, N), BF16)], 2 * RB * N * N * C * 2, "tri_out_bwd")


def finish_body(t_ref, z_ref, lnp_ref, wg_ref, lnq_ref, wo_ref, z_out, st):
    fill(st, t_ref)

    def row(i, carry):
        th, _ = hat_rows(get_row(st, i))
        y = (th * lnq_ref[:, 0:1] + lnq_ref[:, 1:2]).astype(BF16)
        upd = dot(y, wo_ref[...], 0, 0)
        zr = z_ref[i].astype(F32)
        x, _, _ = norm_x(zr, lnp_ref)
        gate = sig(dot(x, wg_ref[...], 1, 0))
        z_out[i] = (zr + gate * upd).astype(BF16)
        return carry

    lax.fori_loop(0, TI, row, 0)


def finish(t, z, lnp, wg, lnq, wo):
    n = RB * N
    return pl.pallas_call(
        finish_body, grid=(RB // TI,),
        in_specs=[chan_spec(), rows_spec(), const_spec((2, C)), const_spec((C, C)), const_spec((C, 2)), const_spec((C, C))],
        out_specs=rows_spec(), out_shape=jax.ShapeDtypeStruct((RB, N, C), BF16), scratch_shapes=[SCR()],
        cost_estimate=cost(n * C * C * 4, n * C * 6, n * C), name="finish",
    )(t, z, lnp, wg, lnq, wo)


def head_body(emit_z, emit_w, t_ref, z_ref, g_ref, lnp_ref, wg_ref, lnq_ref, wo_ref, *rest):
    rest = list(rest)
    st, sd = rest[-2:]
    dt_out, dg_out = rest[0], rest[1]
    k = 2
    if emit_z:
        z_out = rest[k]
        k += 1
    if emit_w:
        gwo, ggain, gshift = rest[k:k + 3]

        @pl.when(pl.program_id(0) == 0)
        def _():
            gwo[...] = jnp.zeros_like(gwo)
            ggain[...] = jnp.zeros_like(ggain)
            gshift[...] = jnp.zeros_like(gshift)

    fill(st, t_ref)

    def row(i, carry):
        th, rstd = hat_rows(get_row(st, i))
        gain = lnq_ref[:, 0:1]
        y = (th * gain + lnq_ref[:, 1:2]).astype(BF16)
        upd = dot(y, wo_ref[...], 0, 0)
        zr = z_ref[i].astype(F32)
        x, _, _ = norm_x(zr, lnp_ref)
        gate = sig(dot(x, wg_ref[...], 1, 0))
        if emit_z:
            z_out[i] = (zr + gate * upd).astype(BF16)
        d = g_ref[i].astype(F32)
        dgate = d * gate
        dg_out[i] = (dgate * upd * (1.0 - gate)).astype(BF16)
        du = dgate.astype(BF16)
        dy = dot(wo_ref[...], du, 1, 1).astype(BF16).astype(F32)
        dh = dy * gain
        m1 = jnp.sum(dh, axis=0, keepdims=True) * (1.0 / C)
        m2 = jnp.sum(dh * th, axis=0, keepdims=True) * (1.0 / C)
        put_row(sd, i, rstd * (dh - m1 - th * m2))
        if emit_w:
            gwo[...] += dot(y, du, 1, 0)
            ggain[...] += dy * th
            gshift[...] += dy
        return carry

    lax.fori_loop(0, TI, row, 0)
    flush(sd, dt_out)


def head(t, z, g, lnp, wg, lnq, wo, emit_z, emit_w):
    n = RB * N
    act = jax.ShapeDtypeStruct((RB, N, C), BF16)
    out_shape = [PART_SHAPE, act]
    out_specs = [chan_spec(), rows_spec()]
    if emit_z:
        out_shape.append(act)
        out_specs.append(rows_spec())
    if emit_w:
        for s in ((C, C), (C, N), (C, N)):
            out_shape.append(jax.ShapeDtypeStruct(s, F32))
            out_specs.append(const_spec(s))
    return pl.pallas_call(
        functools.partial(head_body, emit_z, emit_w), grid=(RB // TI,),
        in_specs=[chan_spec(), rows_spec(), rows_spec(), const_spec((2, C)), const_spec((C, C)), const_spec((C, 2)), const_spec((C, C))],
        out_specs=out_specs, out_shape=out_shape, scratch_shapes=[SCR(), SCR()],
        cost_estimate=cost(n * C * C * 6, n * C * 10, n * C), name="head",
    )(t, z, g, lnp, wg, lnq, wo)


def back_body(emit_w, da_ref, db_ref, z_ref, g_ref, dg_ref, m_ref, lnp_ref, wt_ref, w_ref, wg_ref, d_out, *rest):
    sa, sb = rest[-2:]
    if emit_w:
        gwp, gwg, gln = rest[:3]

        @pl.when(pl.program_id(0) == 0)
        def _():
            gwp[...] = jnp.zeros_like(gwp)
            gwg[...] = jnp.zeros_like(gwg)
            gln[...] = jnp.zeros_like(gln)

    fill(sa, da_ref)
    fill(sb, db_ref)

    def row(i, carry):
        zr = z_ref[i].astype(F32)
        x, xh, rstd = norm_x(zr, lnp_ref)
        p = dot(wt_ref[...], x, 1, 1)
        mrow = m_ref[pl.ds(i, 1), :]
        da = get_row(sa, i) * mrow
        s = sig(p[C:2 * C])
        t0 = da * s
        d0 = t0.astype(BF16)
        d1 = (t0 * p[0:C] * (1.0 - s)).astype(BF16)
        db = get_row(sb, i) * mrow
        s = sig(p[3 * C:4 * C])
        t0 = db * s
        d2 = t0.astype(BF16)
        d3 = (t0 * p[2 * C:3 * C] * (1.0 - s)).astype(BF16)
        dp = jnp.concatenate([d0, d1, d2, d3], axis=0)
        dg = dg_ref[i]
        dxt = dot(w_ref[...], dp, 1, 0) + dot(wg_ref[...], dg, 1, 1)
        dx = dxt.astype(BF16).T.astype(F32)
        dh = dx * lnp_ref[0:1, :]
        m1 = jnp.sum(dh, axis=-1, keepdims=True) * (1.0 / C)
        m2 = jnp.sum(dh * xh, axis=-1, keepdims=True) * (1.0 / C)
        d_out[i] = (g_ref[i].astype(F32) + rstd * (dh - m1 - xh * m2)).astype(BF16)
        if emit_w:
            gwp[...] += dot(dp, x, 1, 0)
            gwg[...] += dot(x, dg, 0, 0)
            gln[0:1, :] += jnp.sum(dx * xh, axis=0, keepdims=True)
            gln[1:2, :] += jnp.sum(dx, axis=0, keepdims=True)
        return carry

    lax.fori_loop(0, TI, row, 0)


def back(da, db, z, g, dg, mask, lnp, wt, w, wg, emit_w):
    n = RB * N
    out_shape = [jax.ShapeDtypeStruct((RB, N, C), BF16)]
    out_specs = [rows_spec()]
    if emit_w:
        for s in ((4 * C, C), (C, C), (2, C)):
            out_shape.append(jax.ShapeDtypeStruct(s, F32))
            out_specs.append(const_spec(s))
    return pl.pallas_call(
        functools.partial(back_body, emit_w), grid=(RB // TI,),
        in_specs=[chan_spec(), chan_spec(), rows_spec(), rows_spec(), rows_spec(), pl.BlockSpec((TI, N), lambda i: (i, 0)),
                  const_spec((2, C)), const_spec((4 * C, C)), const_spec((C, 4 * C)), const_spec((C, C))],
        out_specs=out_specs, out_shape=out_shape, scratch_shapes=[SCR(), SCR()],
        cost_estimate=cost(n * C * C * 20, n * C * 12, n * C * 2), name="back",
    )(da, db, z, g, dg, mask, lnp, wt, w, wg)


def solution(mesh):
    row_spec = P(('data', 'dap'), None, None)
    mask_spec = P(('data', 'dap'), None)
    full_spec = P()
    grad_spec = P('data', None, None)

    def ici(v):
        return lax.ppermute(v, AX, ICI_SWAP)

    def d2d(v):
        return lax.ppermute(v, AX, D2D_SWAP)

    def device_step(pair_act, pair_mask, d_pair_out, ln_pair, w_proj, w_gate, ln_chan, w_out):
        me = lax.axis_index(AX)
        blocks = jnp.stack([me ^ OWN, me ^ CROSS, me ^ PART, me ^ DIAG]).astype(jnp.int32)
        base = [blocks[k:k + 1] * (RB // TI) for k in range(4)]
        lnp = ln_pair.astype(F32)
        lnq = jnp.swapaxes(ln_chan, 1, 2).astype(F32)
        wt = jnp.swapaxes(w_proj, 1, 2)
        m_own = pair_mask.astype(F32)
        m_cross = ici(m_own)
        m_part = d2d(m_own)
        m_diag = d2d(m_cross)
        z_own = pair_act
        z_cross = ici(z_own)
        z_part = d2d(z_own)
        z_diag = d2d(z_cross)
        g_own = d_pair_out
        g_src, z_cross = lax.optimization_barrier((g_own, z_cross))
        g_cross = ici(g_src)

        a1, b1 = prep(base[0], z_own, m_own, lnp[0], wt[0])
        a1, b1 = prep(base[2], z_part, m_part, lnp[0], wt[0], (a1, b1))
        a1, b1 = prep(base[1], z_cross, m_cross, lnp[0], wt[0], (a1, b1))
        a1, b1 = prep(base[3], z_diag, m_diag, lnp[0], wt[0], (a1, b1))
        t1o, t1c = tri_out(blocks, a1, b1)
        y_own = finish(t1o, z_own, lnp[0], w_gate[0], lnq[0], w_out[0])
        y_part = d2d(y_own)
        y_cross = finish(t1c, z_cross, lnp[0], w_gate[0], lnq[0], w_out[0])
        y_diag = d2d(y_cross)

        a2, b2 = prep(base[0], y_own, m_own, lnp[1], wt[1])
        a2, b2 = prep(base[1], y_cross, m_cross, lnp[1], wt[1], (a2, b2))
        a2, b2 = prep(base[2], y_part, m_part, lnp[1], wt[1], (a2, b2))
        a2, b2 = prep(base[3], y_diag, m_diag, lnp[1], wt[1], (a2, b2))
        t2o, t2c = tri_in(blocks, a2, b2)
        dt2o, dg2o, pair_out, gwo2, gq2g, gq2s = head(t2o, y_own, g_own, lnp[1], w_gate[1], lnq[1], w_out[1], True, True)
        dt2p = d2d(dt2o)
        dt2c, dg2c = head(t2c, y_cross, g_cross, lnp[1], w_gate[1], lnq[1], w_out[1], False, False)
        dt2d = d2d(dt2c)
        dao, dac, dbo, dbc = tri_in_bwd(blocks, (dt2o, dt2c, dt2p, dt2d), a2, b2)
        dy_own, gwp2, gwg2, gln2 = back(dao, dbo, y_own, g_own, dg2o, m_own, lnp[1], wt[1], w_proj[1], w_gate[1], True)
        dy_cross, = back(dac, dbc, y_cross, g_cross, dg2c, m_cross, lnp[1], wt[1], w_proj[1], w_gate[1], False)

        dt1o, dg1o, gwo1, gq1g, gq1s = head(t1o, z_own, dy_own, lnp[0], w_gate[0], lnq[0], w_out[0], False, True)
        dt1p = d2d(dt1o)
        dt1c, _ = head(t1c, z_cross, dy_cross, lnp[0], w_gate[0], lnq[0], w_out[0], False, False)
        dt1d = d2d(dt1c)
        da1, db1 = tri_out_bwd(blocks, (dt1o, dt1c, dt1p, dt1d), a1, b1)
        d_pair, gwp1, gwg1, gln1 = back(da1, db1, z_own, dy_own, dg1o, m_own, lnp[0], wt[0], w_proj[0], w_gate[0], True)

        def chan(gg, gs):
            return jnp.stack([jnp.sum(gg, axis=1), jnp.sum(gs, axis=1)])

        local = (jnp.stack([gln1, gln2]),
                 jnp.stack([gwp1.T, gwp2.T]),
                 jnp.stack([gwg1, gwg2]),
                 jnp.stack([chan(gq1g, gq1s), chan(gq2g, gq2s)]),
                 jnp.stack([gwo1, gwo2]))
        sums = lax.psum(local, AX)
        return (pair_out, d_pair) + tuple(v.astype(BF16) for v in sums)

    return jax.shard_map(device_step, mesh=mesh, in_specs=(row_spec, mask_spec, row_spec, full_spec, full_spec, full_spec, full_spec, full_spec), out_specs=(row_spec, row_spec, grad_spec, grad_spec, grad_spec, grad_spec, grad_spec), check_vma=False)
```

```python
import functools
import jax
import jax.numpy as jnp
from jax import lax
from jax.experimental import pallas as pl
from jax.experimental.pallas import tpu as pltpu
from jax.sharding import PartitionSpec as P

LN_EPS = 1e-5
AX = 'dap'
N = 384
C = 128
H = 64
TI = 16
RB = 96
CB = 8
NCH = 2
HC = H // NCH
UNROLL = 4
F32 = jnp.float32
BF16 = jnp.bfloat16
ICI_SWAP = [(0, 2), (2, 0), (1, 3), (3, 1)]
D2D_SWAP = [(0, 1), (1, 0), (2, 3), (3, 2)]
OWN, CROSS, PART, DIAG = 0, 2, 1, 3


def sig(v):
    return 0.5 * jnp.tanh(0.5 * v) + 0.5


def dot(a, b, ca=1, cb=0):
    return lax.dot_general(a, b, (((ca,), (cb,)), ((), ())), preferred_element_type=F32)


def hat(v):
    mean = jnp.sum(v, axis=0, keepdims=True) * (1.0 / C)
    cen = v - mean
    var = jnp.sum(cen * cen, axis=0, keepdims=True) * (1.0 / C)
    rstd = lax.rsqrt(var + LN_EPS)
    return cen * rstd, rstd


def affine(h, ln_ref):
    return (h * ln_ref[:, 0:1] + ln_ref[:, 1:2]).astype(BF16)


def rows_loop(fn, unroll=UNROLL):
    def step(i, carry):
        fn(i)
        return carry
    lax.fori_loop(0, TI, step, 0, unroll=unroll)


def fill(scr, refs):
    at = 0
    for ref in refs:
        for c in range(0, ref.shape[0], 16):
            scr[:, at + c:at + c + 16, :] = jnp.swapaxes(ref[c:c + 16], 0, 1)
        at += ref.shape[0]


def flush(scr, refs):
    at = 0
    for ref in refs:
        for c in range(0, ref.shape[0], 16):
            ref[c:c + 16] = jnp.swapaxes(scr[:, at + c:at + c + 16, :], 0, 1)
        at += ref.shape[0]


def scr(n):
    return pltpu.VMEM((TI, n, N), BF16)


def const_spec(shape):
    nd = len(shape)
    return pl.BlockSpec(shape, lambda *_: (0,) * nd)


def act_spec():
    return pl.BlockSpec((TI, N, C), lambda i, *_: (i, 0, 0))


def actt_spec():
    return pl.BlockSpec((TI, C, N), lambda i, *_: (i, 0, 0))


def mask_spec_():
    return pl.BlockSpec((TI, N), lambda i, *_: (i, 0))


def piece_spec(k, n):
    return pl.BlockSpec((None, n, TI, N), lambda i: (k, 0, i, 0))


def half_spec():
    return pl.BlockSpec((H, TI, N), lambda i: (0, i, 0))


ACT = jax.ShapeDtypeStruct((RB, N, C), BF16)
ACTT = jax.ShapeDtypeStruct((RB, C, N), BF16)
HALF = jax.ShapeDtypeStruct((H, RB, N), BF16)
NPOS = RB * N


def cost(flops, nbytes, trans=0):
    return pl.CostEstimate(flops=int(flops), bytes_accessed=int(nbytes), transcendentals=int(trans))


def turn_body(z_ref, zt_ref):
    def row(i):
        zt_ref[i] = z_ref[i].T
    rows_loop(row)


def turn(z):
    return pl.pallas_call(turn_body, grid=(RB // TI,), in_specs=[act_spec()], out_specs=actt_spec(), out_shape=ACTT,
                          cost_estimate=cost(NPOS * C * 40, NPOS * C * 4), name="turn")(z)


def norm_body(z_ref, ln_ref, zt_ref, xt_ref):
    def row(i):
        zt = z_ref[i].T
        zt_ref[i] = zt
        h, _ = hat(zt.astype(F32))
        xt_ref[i] = affine(h, ln_ref)
    rows_loop(row)


def norm(z, ln):
    return pl.pallas_call(norm_body, grid=(RB // TI,), in_specs=[act_spec(), const_spec((C, 2))], out_specs=[actt_spec()] * 2,
                          out_shape=[ACTT] * 2, cost_estimate=cost(NPOS * C * 60, NPOS * C * 6), name="norm")(z, ln)


def prep_body(base, x_ref, m_ref, wt_ref, *rest):
    a_out, b_out, sa, sb = rest[-4:]

    def row(i):
        mrow = m_ref[pl.ds(i, 1), :]
        p = dot(wt_ref[...], x_ref[i])
        sa[i] = (mrow * sig(p[H:2 * H]) * p[0:H]).astype(BF16)
        sb[i] = (mrow * sig(p[3 * H:4 * H]) * p[2 * H:3 * H]).astype(BF16)

    rows_loop(row)
    flush(sa, [a_out])
    flush(sb, [b_out])


def prep(base, xt, mask, wt, full=None):
    out = jax.ShapeDtypeStruct((H, N, N), BF16)
    spec = pl.BlockSpec((H, TI, N), lambda i, b: (0, b[0] + i, 0))
    extra = () if full is None else tuple(full)
    grid_spec = pltpu.PrefetchScalarGridSpec(
        num_scalar_prefetch=1, grid=(RB // TI,),
        in_specs=[actt_spec(), mask_spec_(), const_spec((4 * H, C))] + [pl.BlockSpec(memory_space=pl.ANY)] * len(extra),
        out_specs=[spec, spec], scratch_shapes=[scr(H), scr(H)])
    return pl.pallas_call(
        prep_body, grid_spec=grid_spec, out_shape=[out, out],
        input_output_aliases={4: 0, 5: 1} if extra else {},
        cost_estimate=cost(NPOS * C * 400, NPOS * C * 4, NPOS * C), name="prep",
    )(base, xt, mask, wt, *extra)


def block_rows(idx, ref, c):
    return [ref[c, pl.ds(pl.multiple_of(idx[k] * RB, RB), RB), :] for k in range(4)]


def emit(vals, keep, send, c):
    keep[0, c] = vals[:RB]
    keep[1, c] = vals[RB:2 * RB]
    send[0, c] = vals[2 * RB:3 * RB]
    send[1, c] = vals[3 * RB:]


def tri_out_body(idx, a, b, keep, send):
    for c in range(CB):
        lhs = jnp.concatenate(block_rows(idx, a, c), axis=0)
        emit(dot(lhs, b[c], 1, 1).astype(BF16), keep, send, c)


def tri_in_body(idx, a, b, keep, send, s):
    for c in range(CB):
        s[c] = a[c].T
        lhs = jnp.concatenate(block_rows(idx, s, c), axis=0)
        emit(dot(lhs, b[c]).astype(BF16), keep, send, c)


def gather_dt(idx, parts, c, s):
    for k, part in enumerate(parts):
        s[c, pl.ds(pl.multiple_of(idx[k] * RB, RB), RB), :] = part[c]


def tri_in_bwd_body(idx, d0, d1, d2, d3, a, b, dak, das, dbk, dbs, s):
    for c in range(CB):
        gather_dt(idx, (d0, d1, d2, d3), c, s)
        emit(dot(jnp.concatenate(block_rows(idx, b, c), axis=0), s[c], 1, 1).astype(BF16), dak, das, c)
        emit(dot(jnp.concatenate(block_rows(idx, a, c), axis=0), s[c]).astype(BF16), dbk, dbs, c)


def tri_out_bwd_body(idx, d0, d1, d2, d3, a, b, dak, das, dbk, dbs, s, st):
    for c in range(CB):
        gather_dt(idx, (d0, d1, d2, d3), c, s)
        da = dot(jnp.concatenate([d0[c], d2[c]], axis=0), b[c]).astype(BF16)
        st[c] = s[c].T
        rows = block_rows(idx, st, c)
        db = dot(jnp.concatenate([rows[0], rows[2]], axis=0), a[c]).astype(BF16)
        dak[0, c] = da[:RB]
        das[0, c] = da[RB:]
        dbk[0, c] = db[:RB]
        dbs[0, c] = db[RB:]


def tri_call(body, idx, part, dts, ab, pieces, n_out, n_scr, flops, name):
    off = part * (HC // CB)
    dspec = pl.BlockSpec((CB, RB, N), lambda c, _: (c + off, 0, 0))
    fspec = pl.BlockSpec((CB, N, N), lambda c, _: (c + off, 0, 0))
    ospec = pl.BlockSpec((pieces, CB, RB, N), lambda c, _: (0, c, 0, 0))
    grid_spec = pltpu.PrefetchScalarGridSpec(
        num_scalar_prefetch=1, grid=(HC // CB,), in_specs=[dspec] * len(dts) + [fspec] * len(ab),
        out_specs=[ospec] * n_out, scratch_shapes=[pltpu.VMEM((CB, N, N), BF16)] * n_scr)
    return pl.pallas_call(body, grid_spec=grid_spec, out_shape=[jax.ShapeDtypeStruct((pieces, HC, RB, N), BF16)] * n_out,
                          cost_estimate=cost(flops, 50e6), name=name)(idx, *dts, *ab)


def finish_body(*refs):
    ts = refs[:2 * NCH]
    z_ref, x_ref, wg_ref, lnq_ref, wo_ref, ln_ref, z_out, x_out, st = refs[2 * NCH:]
    fill(st, ts)

    def row(i):
        th, _ = hat(st[i].astype(F32))
        upd = dot(wo_ref[...], affine(th, lnq_ref))
        gate = sig(dot(wg_ref[...], x_ref[i]))
        zn = (z_ref[i].astype(F32) + gate * upd).astype(BF16)
        z_out[i] = zn
        h, _ = hat(zn.astype(F32))
        x_out[i] = affine(h, ln_ref)

    rows_loop(row)


def finish(k, ts, zt, xt, wgt, lnq, wot, ln_next):
    return pl.pallas_call(
        finish_body, grid=(RB // TI,),
        in_specs=[piece_spec(k, HC)] * (2 * NCH) + [actt_spec(), actt_spec(), const_spec((C, C)), const_spec((C, 2)), const_spec((C, C)), const_spec((C, 2))],
        out_specs=[actt_spec()] * 2, out_shape=[ACTT] * 2, scratch_shapes=[scr(C)],
        cost_estimate=cost(NPOS * C * 600, NPOS * C * 10, NPOS * C), name="finish",
    )(*ts, zt, xt, wgt, lnq, wot, ln_next)


def head_body(emit_z, emit_w, *refs):
    ts = refs[:2 * NCH]
    refs = list(refs[2 * NCH:])
    x_ref, g_ref, wg_ref, lnq_ref, wot_ref, wo_ref = refs[:6]
    k = 6
    if emit_z:
        z_ref = refs[k]
        k += 1
    dt_keep, dt_send, dg_out = refs[k:k + 3]
    k += 3
    if emit_z:
        z_out = refs[k]
        k += 1
    if emit_w:
        gwo, ggain, gshift = refs[k:k + 3]

        @pl.when(pl.program_id(0) == 0)
        def _():
            gwo[...] = jnp.zeros_like(gwo)
            ggain[...] = jnp.zeros_like(ggain)
            gshift[...] = jnp.zeros_like(gshift)

    st, sd = refs[-2:]
    fill(st, ts)

    def row(i):
        th, rstd = hat(st[i].astype(F32))
        y = affine(th, lnq_ref)
        upd = dot(wot_ref[...], y)
        gate = sig(dot(wg_ref[...], x_ref[i]))
        if emit_z:
            z_out[i] = (z_ref[i].astype(F32) + gate * upd).astype(BF16).T
        dgate = g_ref[i].astype(F32) * gate
        dg_out[i] = (dgate * upd * (1.0 - gate)).astype(BF16)
        du = dgate.astype(BF16)
        dy = dot(wo_ref[...], du).astype(BF16).astype(F32)
        dh = dy * lnq_ref[:, 0:1]
        m1 = jnp.sum(dh, axis=0, keepdims=True) * (1.0 / C)
        m2 = jnp.sum(dh * th, axis=0, keepdims=True) * (1.0 / C)
        sd[i] = (rstd * (dh - m1 - th * m2)).astype(BF16)
        if emit_w:
            gwo[...] += dot(y, du, 1, 1)
            e = dy * th
            ggain[...] += e[:, 0:128] + e[:, 128:256] + e[:, 256:384]
            gshift[...] += dy[:, 0:128] + dy[:, 128:256] + dy[:, 256:384]

    rows_loop(row)
    flush(sd, [dt_keep, dt_send])


def head(k, ts, xt, gt, wgt, lnq, wot, wo, zt=None, emit_w=False):
    emit_z = zt is not None
    in_specs = [piece_spec(k, HC)] * (2 * NCH) + [actt_spec(), actt_spec(), const_spec((C, C)), const_spec((C, 2)), const_spec((C, C)), const_spec((C, C))]
    out_shape = [HALF, HALF, ACTT]
    out_specs = [half_spec(), half_spec(), actt_spec()]
    extra = ()
    if emit_z:
        in_specs.append(actt_spec())
        extra = (zt,)
        out_shape.append(ACT)
        out_specs.append(act_spec())
    if emit_w:
        for s in ((C, C), (C, C), (C, C)):
            out_shape.append(jax.ShapeDtypeStruct(s, F32))
            out_specs.append(const_spec(s))
    return pl.pallas_call(
        functools.partial(head_body, emit_z, emit_w), grid=(RB // TI,), in_specs=in_specs,
        out_specs=out_specs, out_shape=out_shape, scratch_shapes=[scr(C), scr(C)],
        cost_estimate=cost(NPOS * C * 800, NPOS * C * 10, NPOS * C), name="head",
    )(*ts, xt, gt, wgt, lnq, wot, wo, *extra)


def back_body(n_ab, emit_w, last, *refs):
    das, dbs = refs[:n_ab], refs[n_ab:2 * n_ab]
    refs = refs[2 * n_ab:]
    z_ref, g_ref, dg_ref, m_ref, ln_ref, wt_ref, wb_ref, d_out = refs[:8]
    if emit_w:
        gw, ggain, gshift = refs[8:11]

        @pl.when(pl.program_id(0) == 0)
        def _():
            gw[...] = jnp.zeros_like(gw)
            ggain[...] = jnp.zeros_like(ggain)
            gshift[...] = jnp.zeros_like(gshift)

    sa, sb = refs[-2:]
    fill(sa, das)
    fill(sb, dbs)

    def row(i):
        xh, rstd = hat(z_ref[i].astype(F32))
        x = affine(xh, ln_ref)
        mrow = m_ref[pl.ds(i, 1), :]
        ds = []
        for s, at in ((sa, 0), (sb, 2 * C)):
            p = dot(wt_ref[at:at + 2 * C], x)
            sg = sig(p[C:])
            t0 = s[i].astype(F32) * mrow * sg
            ds.append(t0.astype(BF16))
            ds.append((t0 * p[:C] * (1.0 - sg)).astype(BF16))
        dp = jnp.concatenate(ds + [dg_ref[i]], axis=0)
        dx = dot(wb_ref[...], dp).astype(BF16).astype(F32)
        dh = dx * ln_ref[:, 0:1]
        m1 = jnp.sum(dh, axis=0, keepdims=True) * (1.0 / C)
        m2 = jnp.sum(dh * xh, axis=0, keepdims=True) * (1.0 / C)
        d = (g_ref[i].astype(F32) + rstd * (dh - m1 - xh * m2)).astype(BF16)
        d_out[i] = d.T if last else d
        if emit_w:
            gw[...] += dot(dp, x, 1, 1)
            e = dx * xh
            ggain[...] += e[:, 0:128] + e[:, 128:256] + e[:, 256:384]
            gshift[...] += dx[:, 0:128] + dx[:, 128:256] + dx[:, 256:384]

    rows_loop(row)


def back(k, das, dbs, zt, gt, dgt, mask, ln, wt, wb, emit_w, last):
    n = len(das)
    out_shape = [ACT if last else ACTT]
    out_specs = [act_spec() if last else actt_spec()]
    if emit_w:
        for s in ((5 * C, C), (C, C), (C, C)):
            out_shape.append(jax.ShapeDtypeStruct(s, F32))
            out_specs.append(const_spec(s))
    return pl.pallas_call(
        functools.partial(back_body, n, emit_w, last), grid=(RB // TI,),
        in_specs=[piece_spec(k, HC)] * (2 * n) + [actt_spec()] * 3 + [mask_spec_(), const_spec((C, 2)), const_spec((4 * C, C)), const_spec((C, 5 * C))],
        out_specs=out_specs, out_shape=out_shape, scratch_shapes=[scr(C), scr(C)],
        cost_estimate=cost(NPOS * C * 2000, NPOS * C * 12, NPOS * C * 2), name="back",
    )(*das, *dbs, zt, gt, dgt, mask, ln, wt, wb)


def solution(mesh):
    row_spec = P(('data', 'dap'), None, None)
    mask_spec = P(('data', 'dap'), None)
    full_spec = P()
    grad_spec = P('data', None, None)

    def ici(v):
        return lax.ppermute(v, AX, ICI_SWAP)

    def d2d(v):
        return lax.ppermute(v, AX, D2D_SWAP)

    def device_step(pair_act, pair_mask, d_pair_out, ln_pair, w_proj, w_gate, ln_chan, w_out):
        me = lax.axis_index(AX)
        odd = (me & 1) == 1
        blocks = jnp.stack([me ^ OWN, me ^ CROSS, me ^ PART, me ^ DIAG]).astype(jnp.int32)
        base = [blocks[k:k + 1] * (RB // TI) for k in range(4)]

        def local(v, axis):
            return jnp.where(odd, jnp.roll(v, H, axis=axis), v)

        m_own = pair_mask.astype(F32)
        m_cross = ici(m_own)
        m_part = d2d(m_own)
        m_diag = d2d(m_cross)
        z_cross = ici(pair_act)

        ln = [ln_pair[u].T.astype(F32) for u in range(2)]
        lnq = [local(ln_chan[u].T.astype(F32), 0) for u in range(2)]
        wp4 = [local(w_proj[u].reshape(C, 4, C), 2) for u in range(2)]
        wt_half = [wp4[u][:, :, :H].reshape(C, 4 * H).T for u in range(2)]
        wt = [wp4[u].reshape(C, 4 * C).T for u in range(2)]
        wb = [jnp.concatenate([wp4[u].reshape(C, 4 * C), w_gate[u]], axis=1) for u in range(2)]
        wgt = [w_gate[u].T for u in range(2)]
        wo = [local(w_out[u], 0) for u in range(2)]
        wot = [wo[u].T for u in range(2)]

        def products(body, name, dts, a, b, pieces, n_scr, flops):
            n_out = 4 if dts else 2
            res = [tri_call(body, blocks, part, dts, (a, b), pieces, n_out, n_scr, flops / NCH, name) for part in range(NCH)]
            keeps = [[r[j] for r in res] for j in range(0, n_out, 2)]
            sends = [[d2d(r[j]) for r in res] for j in range(1, n_out, 2)]
            return [k + s for k, s in zip(keeps, sends)]

        zt_own, xt_own = norm(pair_act, ln[0])
        xt_part = d2d(xt_own)
        gt_own = turn(d_pair_out)
        ab1 = prep(base[0], xt_own, m_own, wt_half[0])
        ab1 = prep(base[2], xt_part, m_part, wt_half[0], ab1)
        gt_src, z_cross, a1, b1 = lax.optimization_barrier((gt_own, z_cross, ab1[0], ab1[1]))
        gt_cross = ici(gt_src)
        zt_cross, xt_cross = norm(z_cross, ln[0])
        xt_diag = d2d(xt_cross)
        ab1 = prep(base[1], xt_cross, m_cross, wt_half[0], (a1, b1))
        a1, b1 = prep(base[3], xt_diag, m_diag, wt_half[0], ab1)
        t1, = products(tri_out_body, "tri_out", (), a1, b1, 2, 0, 7.2e9)
        yt_own, vt_own = finish(0, t1, zt_own, xt_own, wgt[0], lnq[0], wot[0], ln[1])
        vt_part = d2d(vt_own)
        yt_cross, vt_cross = finish(1, t1, zt_cross, xt_cross, wgt[0], lnq[0], wot[0], ln[1])
        vt_diag = d2d(vt_cross)

        ab2 = prep(base[0], vt_own, m_own, wt_half[1])
        ab2 = prep(base[2], vt_part, m_part, wt_half[1], ab2)
        ab2 = prep(base[1], vt_cross, m_cross, wt_half[1], ab2)
        a2, b2 = prep(base[3], vt_diag, m_diag, wt_half[1], ab2)
        t2, = products(tri_in_body, "tri_in", (), a2, b2, 2, 1, 7.2e9)

        dk_own, ds_own, dg2_own, pair_out, gwo2, gq2g, gq2s = head(0, t2, vt_own, gt_own, wgt[1], lnq[1], wot[1], wo[1], yt_own, True)
        dk_part = d2d(ds_own)
        dk_cross, ds_cross, dg2_cross = head(1, t2, vt_cross, gt_cross, wgt[1], lnq[1], wot[1], wo[1])
        dk_diag = d2d(ds_cross)
        da2, db2 = products(tri_in_bwd_body, "tri_in_bwd", (dk_own, dk_cross, dk_part, dk_diag), a2, b2, 2, 1, 14.4e9)
        et_own, gw2, gp2g, gp2s = back(0, da2, db2, yt_own, gt_own, dg2_own, m_own, ln[1], wt[1], wb[1], True, False)
        et_cross, = back(1, da2, db2, yt_cross, gt_cross, dg2_cross, m_cross, ln[1], wt[1], wb[1], False, False)

        dk_own, ds_own, dg1_own, gwo1, gq1g, gq1s = head(0, t1, xt_own, et_own, wgt[0], lnq[0], wot[0], wo[0], None, True)
        dk_part = d2d(ds_own)
        dk_cross, ds_cross, _ = head(1, t1, xt_cross, et_cross, wgt[0], lnq[0], wot[0], wo[0])
        dk_diag = d2d(ds_cross)
        da1, db1 = products(tri_out_bwd_body, "tri_out_bwd", (dk_own, dk_cross, dk_part, dk_diag), a1, b1, 1, 2, 7.2e9)
        d_pair, gw1, gp1g, gp1s = back(0, da1, db1, zt_own, et_own, dg1_own, m_own, ln[0], wt[0], wb[0], True, True)

        def vec(gg, gs):
            return jnp.stack([jnp.sum(gg, axis=1), jnp.sum(gs, axis=1)])

        def proj(g):
            return local(g[:4 * C].T.reshape(C, 4, C), 2).reshape(C, 4 * C)

        grads = (jnp.stack([vec(gp1g, gp1s), vec(gp2g, gp2s)]),
                 jnp.stack([proj(gw1), proj(gw2)]),
                 jnp.stack([gw1[4 * C:].T, gw2[4 * C:].T]),
                 jnp.stack([local(vec(gq1g, gq1s), 1), local(vec(gq2g, gq2s), 1)]),
                 jnp.stack([local(gwo1, 0), local(gwo2, 0)]))
        sums = lax.psum(grads, AX)
        return (pair_out, d_pair) + tuple(v.astype(BF16) for v in sums)

    return jax.shard_map(device_step, mesh=mesh, in_specs=(row_spec, mask_spec, row_spec, full_spec, full_spec, full_spec, full_spec, full_spec), out_specs=(row_spec, row_spec, grad_spec, grad_spec, grad_spec, grad_spec, grad_spec), check_vma=False)
```

```python
import functools
import jax
import jax.numpy as jnp
from jax import lax
from jax.experimental import pallas as pl
from jax.experimental.pallas import tpu as pltpu
from jax.sharding import PartitionSpec as P

LN_EPS = 1e-5
AX = 'dap'
N = 384
C = 128
H = 64
TI = 16
RB = 96
CB = 8
NCH = 2
HC = H // NCH
UNROLL = 2
G = 2
ZC = 3
ZR = RB // ZC
F32 = jnp.float32
BF16 = jnp.bfloat16
ICI_SWAP = [(0, 2), (2, 0), (1, 3), (3, 1)]
D2D_SWAP = [(0, 1), (1, 0), (2, 3), (3, 2)]
OWN, CROSS, PART, DIAG = 0, 2, 1, 3


def dot(a, b, ca=1, cb=0):
    return lax.dot_general(a, b, (((ca,), (cb,)), ((), ())), preferred_element_type=F32)


def hat(v):
    mean = jnp.sum(v, axis=0, keepdims=True) * (1.0 / C)
    cen = v - mean
    var = jnp.sum(cen * cen, axis=0, keepdims=True) * (1.0 / C)
    rstd = lax.rsqrt(var + LN_EPS)
    return cen * rstd, rstd


def affine(h, ln_ref):
    return (h * ln_ref[:, 0:1] + ln_ref[:, 1:2]).astype(BF16)


def rows_loop(fn, unroll=UNROLL, n=TI // G):
    def step(i, carry):
        fn(i)
        return carry

    lax.fori_loop(0, n, step, 0, unroll=unroll)


def get(ref, i):
    return jnp.concatenate([ref[G * i + r] for r in range(G)], axis=1)


def put(ref, i, v):
    for r in range(G):
        ref[G * i + r] = v[:, r * N:(r + 1) * N]


def put_turned(ref, i, v):
    for r in range(G):
        ref[G * i + r] = v[:, r * N:(r + 1) * N].T


def get_mask(ref, i):
    return jnp.concatenate([ref[pl.ds(G * i + r, 1), :] for r in range(G)], axis=1).astype(BF16)


def fold(v):
    return functools.reduce(lambda p, q: p + q, [v[:, k * 128:(k + 1) * 128] for k in range(G * N // 128)])


def fill(scr, refs):
    at = 0
    for ref in refs:
        for c in range(0, ref.shape[0], 16):
            scr[:, at + c:at + c + 16, :] = jnp.swapaxes(ref[c:c + 16], 0, 1)
        at += ref.shape[0]


def flush(scr, refs):
    at = 0
    for ref in refs:
        for c in range(0, ref.shape[0], 16):
            ref[c:c + 16] = jnp.swapaxes(scr[:, at + c:at + c + 16, :], 0, 1)
        at += ref.shape[0]


def scr(n):
    return pltpu.VMEM((TI, n, N), BF16)


def const_spec(shape):
    nd = len(shape)
    return pl.BlockSpec(shape, lambda *_: (0,) * nd)


def act_spec():
    return pl.BlockSpec((TI, N, C), lambda i, *_: (i, 0, 0))


def actt_spec():
    return pl.BlockSpec((TI, C, N), lambda i, *_: (i, 0, 0))


def mask_spec_():
    return pl.BlockSpec((TI, N), lambda i, *_: (i, 0))


def piece_spec(k, n):
    return pl.BlockSpec((None, n, TI, N), lambda i: (k, 0, i, 0))


def half_spec():
    return pl.BlockSpec((H, TI, N), lambda i: (0, i, 0))


ACT = jax.ShapeDtypeStruct((RB, N, C), BF16)
ACTT = jax.ShapeDtypeStruct((RB, C, N), BF16)
HALF = jax.ShapeDtypeStruct((H, RB, N), BF16)
NPOS = RB * N


def cost(flops, nbytes, trans=0):
    return pl.CostEstimate(flops=int(flops), bytes_accessed=int(nbytes), transcendentals=int(trans))


def turn_body(z_ref, zt_ref):
    rows_loop(lambda i: put(zt_ref, i, jnp.concatenate([z_ref[G * i + r].T for r in range(G)], axis=1)))


def turn(z):
    return pl.pallas_call(turn_body, grid=(RB // TI,), in_specs=[act_spec()], out_specs=actt_spec(), out_shape=ACTT,
                          cost_estimate=cost(NPOS * C * 40, NPOS * C * 4), name="turn")(z)


def norm_body(z_ref, ln_ref, *rest):
    zt_ref, xt_ref, xc_ref = rest[-3:]

    def row(i):
        zt = jnp.concatenate([z_ref[G * i + r].T for r in range(G)], axis=1)
        put(zt_ref, i, zt)
        h, _ = hat(zt.astype(F32))
        x = affine(h, ln_ref)
        put(xt_ref, i, x)
        put(xc_ref, i, x)

    rows_loop(row)


def norm(z, ln, part=0, full=None):
    rows = z.shape[0]
    off = part * (ZR // TI)
    extra = () if full is None else tuple(full)
    spec = pl.BlockSpec((TI, C, N), lambda i: (i + off, 0, 0))
    return pl.pallas_call(norm_body, grid=(rows // TI,), in_specs=[act_spec(), const_spec((C, 2))] + [pl.BlockSpec(memory_space=pl.ANY)] * len(extra),
                          out_specs=[spec, spec, actt_spec()], out_shape=[ACTT, ACTT, jax.ShapeDtypeStruct((rows, C, N), BF16)],
                          input_output_aliases={2: 0, 3: 1} if extra else {},
                          cost_estimate=cost(rows * N * C * 60, rows * N * C * 8), name="norm")(z, ln, *extra)


def prep_body(base, x_ref, m_ref, wt_ref, *rest):
    a_out, b_out, sa, sb = rest[-4:]

    def row(i):
        p = dot(wt_ref[...], get(x_ref, i) * get_mask(m_ref, i))
        for out, at in ((sa, 0), (sb, 2 * H)):
            lin = p[at:at + H]
            put(out, i, (lin * jnp.tanh(p[at + H:at + 2 * H]) + lin).astype(BF16))

    rows_loop(row)
    flush(sa, [a_out])
    flush(sb, [b_out])


def prep(base, xt, mask, wt, full=None):
    rows = xt.shape[0]
    npos = rows * N
    out = jax.ShapeDtypeStruct((H, N, N), BF16)
    spec = pl.BlockSpec((H, TI, N), lambda i, b: (0, b[0] + i, 0))
    extra = () if full is None else tuple(full)
    grid_spec = pltpu.PrefetchScalarGridSpec(
        num_scalar_prefetch=1, grid=(rows // TI,),
        in_specs=[actt_spec(), mask_spec_(), const_spec((4 * H, C))] + [pl.BlockSpec(memory_space=pl.ANY)] * len(extra),
        out_specs=[spec, spec], scratch_shapes=[scr(H), scr(H)])
    return pl.pallas_call(
        prep_body, grid_spec=grid_spec, out_shape=[out, out],
        input_output_aliases={4: 0, 5: 1} if extra else {},
        cost_estimate=cost(npos * C * 400, npos * C * 4, npos * C), name="prep",
    )(base, xt, mask, wt, *extra)


def block_rows(idx, ref, c):
    return [ref[c, pl.ds(pl.multiple_of(idx[k] * RB, RB), RB), :] for k in range(4)]


def emit(vals, keep, send, c):
    keep[0, c] = vals[:RB]
    keep[1, c] = vals[RB:2 * RB]
    send[0, c] = vals[2 * RB:3 * RB]
    send[1, c] = vals[3 * RB:]


def tri_out_body(idx, a, b, keep, send):
    def chan(c):
        lhs = jnp.concatenate(block_rows(idx, a, c), axis=0)
        emit(dot(lhs, b[c], 1, 1).astype(BF16), keep, send, c)

    rows_loop(chan, 2, CB)


def tri_in_body(idx, a, b, keep, send, s):
    def chan(c):
        s[c] = a[c].T
        lhs = jnp.concatenate(block_rows(idx, s, c), axis=0)
        emit(dot(lhs, b[c]).astype(BF16), keep, send, c)

    rows_loop(chan, 2, CB)


def gather_dt(idx, parts, c, s):
    for k, part in enumerate(parts):
        s[c, pl.ds(pl.multiple_of(idx[k] * RB, RB), RB), :] = part[c]


def tri_in_bwd_body(idx, d0, d1, d2, d3, a, b, dak, das, dbk, dbs, s):
    def chan(c):
        gather_dt(idx, (d0, d1, d2, d3), c, s)
        emit(dot(jnp.concatenate(block_rows(idx, b, c), axis=0), s[c], 1, 1).astype(BF16), dak, das, c)
        emit(dot(jnp.concatenate(block_rows(idx, a, c), axis=0), s[c]).astype(BF16), dbk, dbs, c)

    rows_loop(chan, 2, CB)


def tri_out_bwd_body(idx, d0, d1, d2, d3, a, b, dak, das, dbk, dbs, s, st):
    def chan(c):
        gather_dt(idx, (d0, d1, d2, d3), c, s)
        da = dot(jnp.concatenate([d0[c], d2[c]], axis=0), b[c]).astype(BF16)
        st[c] = s[c].T
        rows = block_rows(idx, st, c)
        db = dot(jnp.concatenate([rows[0], rows[2]], axis=0), a[c]).astype(BF16)
        dak[0, c] = da[:RB]
        das[0, c] = da[RB:]
        dbk[0, c] = db[:RB]
        dbs[0, c] = db[RB:]

    rows_loop(chan, 2, CB)


def tri_call(body, idx, part, dts, ab, pieces, n_out, n_scr, flops):
    off = part * (HC // CB)
    dspec = pl.BlockSpec((CB, RB, N), lambda c, _: (c + off, 0, 0))
    fspec = pl.BlockSpec((CB, N, N), lambda c, _: (c + off, 0, 0))
    ospec = pl.BlockSpec((pieces, CB, RB, N), lambda c, _: (0, c, 0, 0))
    grid_spec = pltpu.PrefetchScalarGridSpec(
        num_scalar_prefetch=1, grid=(HC // CB,), in_specs=[dspec] * len(dts) + [fspec] * len(ab),
        out_specs=[ospec] * n_out, scratch_shapes=[pltpu.VMEM((CB, N, N), BF16)] * n_scr)
    return pl.pallas_call(body, grid_spec=grid_spec, out_shape=[jax.ShapeDtypeStruct((pieces, HC, RB, N), BF16)] * n_out,
                          cost_estimate=cost(flops, 50e6))(idx, *dts, *ab)


def finish_body(*refs):
    ts = refs[:2 * NCH]
    z_ref, x_ref, wg_ref, lnq_ref, wo_ref, ln_ref, z_out, x_out, st = refs[2 * NCH:]
    fill(st, ts)

    def row(i):
        th, _ = hat(get(st, i).astype(F32))
        upd = dot(wo_ref[...], affine(th, lnq_ref))
        gate = jnp.tanh(dot(wg_ref[...], get(x_ref, i)))
        zn = (get(z_ref, i).astype(F32) + (gate * upd + upd)).astype(BF16)
        put(z_out, i, zn)
        h, _ = hat(zn.astype(F32))
        put(x_out, i, affine(h, ln_ref))

    rows_loop(row)


def finish(k, ts, zt, xt, wgt, lnq, wot, ln_next):
    return pl.pallas_call(
        finish_body, grid=(RB // TI,),
        in_specs=[piece_spec(k, HC)] * (2 * NCH) + [actt_spec(), actt_spec(), const_spec((C, C)), const_spec((C, 2)), const_spec((C, C)), const_spec((C, 2))],
        out_specs=[actt_spec()] * 2, out_shape=[ACTT] * 2, scratch_shapes=[scr(C)],
        cost_estimate=cost(NPOS * C * 600, NPOS * C * 10, NPOS * C), name="finish",
    )(*ts, zt, xt, wgt, lnq, wot, ln_next)


def head_body(emit_z, emit_w, *refs):
    ts = refs[:2 * NCH]
    refs = list(refs[2 * NCH:])
    x_ref, g_ref, wg_ref, lnq_ref, wot_ref, wo_ref = refs[:6]
    k = 6
    if emit_z:
        z_ref = refs[k]
        k += 1
    dt_keep, dt_send, dg_out = refs[k:k + 3]
    k += 3
    if emit_z:
        z_out = refs[k]
        k += 1
    if emit_w:
        gwo, ggain, gshift = refs[k:k + 3]

        @pl.when(pl.program_id(0) == 0)
        def _():
            gwo[...] = jnp.zeros_like(gwo)
            ggain[...] = jnp.zeros_like(ggain)
            gshift[...] = jnp.zeros_like(gshift)

    st, sd = refs[-2:]
    fill(st, ts)

    def row(i):
        th, rstd = hat(get(st, i).astype(F32))
        y = affine(th, lnq_ref)
        upd = dot(wot_ref[...], y)
        gate = jnp.tanh(dot(wg_ref[...], get(x_ref, i)))
        if emit_z:
            put_turned(z_out, i, (get(z_ref, i).astype(F32) + (gate * upd + upd)).astype(BF16))
        dgate = get(g_ref, i).astype(F32) * (0.5 * gate + 0.5)
        put(dg_out, i, (dgate * (upd - upd * gate)).astype(BF16))
        du = dgate.astype(BF16)
        dy = dot(wo_ref[...], du).astype(BF16).astype(F32)
        dh = dy * lnq_ref[:, 0:1]
        m1 = jnp.sum(dh, axis=0, keepdims=True) * (1.0 / C)
        m2 = jnp.sum(dh * th, axis=0, keepdims=True) * (1.0 / C)
        put(sd, i, (rstd * (dh - m1 - th * m2)).astype(BF16))
        if emit_w:
            gwo[...] += dot(y, du, 1, 1)
            ggain[...] += fold(dy * th)
            gshift[...] += fold(dy)

    rows_loop(row)
    flush(sd, [dt_keep, dt_send])


def head(k, ts, xt, gt, wgt, lnq, wot, wo, zt=None, emit_w=False):
    emit_z = zt is not None
    in_specs = [piece_spec(k, HC)] * (2 * NCH) + [actt_spec(), actt_spec(), const_spec((C, C)), const_spec((C, 2)), const_spec((C, C)), const_spec((C, C))]
    out_shape = [HALF, HALF, ACTT]
    out_specs = [half_spec(), half_spec(), actt_spec()]
    extra = ()
    if emit_z:
        in_specs.append(actt_spec())
        extra = (zt,)
        out_shape.append(ACT)
        out_specs.append(act_spec())
    if emit_w:
        for s in ((C, C), (C, C), (C, C)):
            out_shape.append(jax.ShapeDtypeStruct(s, F32))
            out_specs.append(const_spec(s))
    return pl.pallas_call(
        functools.partial(head_body, emit_z, emit_w), grid=(RB // TI,), in_specs=in_specs,
        out_specs=out_specs, out_shape=out_shape, scratch_shapes=[scr(C), scr(C)],
        cost_estimate=cost(NPOS * C * 800, NPOS * C * 10, NPOS * C), name="head",
    )(*ts, xt, gt, wgt, lnq, wot, wo, *extra)


def back_body(n_ab, emit_w, last, *refs):
    das, dbs = refs[:n_ab], refs[n_ab:2 * n_ab]
    refs = refs[2 * n_ab:]
    z_ref, g_ref, dg_ref, m_ref, ln_ref, wt_ref, wb_ref, d_out = refs[:8]
    if emit_w:
        gw, ggain, gshift = refs[8:11]

        @pl.when(pl.program_id(0) == 0)
        def _():
            gw[...] = jnp.zeros_like(gw)
            ggain[...] = jnp.zeros_like(ggain)
            gshift[...] = jnp.zeros_like(gshift)

    sa, sb = refs[-2:]
    fill(sa, das)
    fill(sb, dbs)

    def row(i):
        xh, rstd = hat(get(z_ref, i).astype(F32))
        x = affine(xh, ln_ref)
        mrow = get_mask(m_ref, i)
        ds = []
        for s, at in ((sa, 0), (sb, 2 * C)):
            p = dot(wt_ref[at:at + 2 * C], x)
            th = jnp.tanh(p[C:])
            t0 = (get(s, i) * mrow).astype(F32) * (0.5 * th + 0.5)
            ds.append(t0.astype(BF16))
            ds.append((t0 * (p[:C] - p[:C] * th)).astype(BF16))
        dp = jnp.concatenate(ds + [get(dg_ref, i)], axis=0)
        dx = dot(wb_ref[...], dp).astype(BF16).astype(F32)
        dh = dx * ln_ref[:, 0:1]
        m1 = jnp.sum(dh, axis=0, keepdims=True) * (1.0 / C)
        m2 = jnp.sum(dh * xh, axis=0, keepdims=True) * (1.0 / C)
        d = (get(g_ref, i).astype(F32) + rstd * (dh - m1 - xh * m2)).astype(BF16)
        (put_turned if last else put)(d_out, i, d)
        if emit_w:
            gw[...] += dot(dp, x, 1, 1)
            ggain[...] += fold(dx * xh)
            gshift[...] += fold(dx)

    rows_loop(row)


def back(k, das, dbs, zt, gt, dgt, mask, ln, wt, wb, emit_w, last):
    n = len(das)
    out_shape = [ACT if last else ACTT]
    out_specs = [act_spec() if last else actt_spec()]
    if emit_w:
        for s in ((5 * C, C), (C, C), (C, C)):
            out_shape.append(jax.ShapeDtypeStruct(s, F32))
            out_specs.append(const_spec(s))
    return pl.pallas_call(
        functools.partial(back_body, n, emit_w, last), grid=(RB // TI,),
        in_specs=[piece_spec(k, HC)] * (2 * n) + [actt_spec()] * 3 + [mask_spec_(), const_spec((C, 2)), const_spec((4 * C, C)), const_spec((C, 5 * C))],
        out_specs=out_specs, out_shape=out_shape, scratch_shapes=[scr(C), scr(C)],
        cost_estimate=cost(NPOS * C * 2000, NPOS * C * 12, NPOS * C * 2), name="back",
    )(*das, *dbs, zt, gt, dgt, mask, ln, wt, wb)


def solution(mesh):
    row_spec = P(('data', 'dap'), None, None)
    mask_spec = P(('data', 'dap'), None)
    full_spec = P()
    grad_spec = P('data', None, None)

    def ici(v):
        return lax.ppermute(v, AX, ICI_SWAP)

    def d2d(v):
        return lax.ppermute(v, AX, D2D_SWAP)

    def device_step(pair_act, pair_mask, d_pair_out, ln_pair, w_proj, w_gate, ln_chan, w_out):
        me = lax.axis_index(AX)
        odd = (me & 1) == 1
        blocks = jnp.stack([me ^ OWN, me ^ CROSS, me ^ PART, me ^ DIAG]).astype(jnp.int32)
        base = [blocks[k:k + 1] * (RB // TI) for k in range(4)]

        def local(v, axis):
            return jnp.where(odd, jnp.roll(v, H, axis=axis), v)

        m_own = pair_mask.astype(F32)
        m_cross = ici(m_own)
        m_part = d2d(m_own)
        m_diag = d2d(m_cross)

        ln = [ln_pair[u].T.astype(F32) for u in range(2)]
        lnq = [local(ln_chan[u].T.astype(F32), 0) for u in range(2)]
        wp4 = [local(w_proj[u].reshape(C, 4, C), 2) for u in range(2)]
        wt_half = [(0.5 * wp4[u][:, :, :H]).reshape(C, 4 * H).T for u in range(2)]
        wt = [(0.5 * wp4[u]).reshape(C, 4 * C).T for u in range(2)]
        wb = [jnp.concatenate([wp4[u].reshape(C, 4 * C), w_gate[u]], axis=1) for u in range(2)]
        wgt = [0.5 * w_gate[u].T for u in range(2)]
        wo = [local(w_out[u], 0) for u in range(2)]
        wot = [0.5 * wo[u].T for u in range(2)]

        def products(body, dts, a, b, pieces, n_scr, flops):
            n_out = 4 if dts else 2
            res = [tri_call(body, blocks, part, dts, (a, b), pieces, n_out, n_scr, flops / NCH) for part in range(NCH)]
            keeps = [[r[j] for r in res] for j in range(0, n_out, 2)]
            sends = [[d2d(r[j]) for r in res] for j in range(1, n_out, 2)]
            return [k + s for k, s in zip(keeps, sends)]

        z_parts = []
        for j in range(ZC):
            z_parts.append(ici(pair_act[j * ZR:(j + 1) * ZR]))
        zt_own, xt_own, _ = norm(pair_act, ln[0])
        xt_part = d2d(xt_own)
        gt_own = turn(d_pair_out)
        gt_cross = ici(gt_own)
        ab1 = prep(base[0], xt_own, m_own, wt_half[0])
        ab1 = prep(base[2], xt_part, m_part, wt_half[0], ab1)
        full = None
        for j in range(ZC):
            zt_cross, xt_cross, xc = norm(z_parts[j], ln[0], j, full)
            full = (zt_cross, xt_cross)
            xd = d2d(xc)
            rows = slice(j * ZR, (j + 1) * ZR)
            ab1 = prep(base[1] + j * (ZR // TI), xc, m_cross[rows], wt_half[0], ab1)
            ab1 = prep(base[3] + j * (ZR // TI), xd, m_diag[rows], wt_half[0], ab1)
        a1, b1 = ab1
        t1, = products(tri_out_body, (), a1, b1, 2, 0, 7.2e9)
        yt_own, vt_own = finish(0, t1, zt_own, xt_own, wgt[0], lnq[0], wot[0], ln[1])
        vt_part = d2d(vt_own)
        yt_cross, vt_cross = finish(1, t1, zt_cross, xt_cross, wgt[0], lnq[0], wot[0], ln[1])
        vt_diag = d2d(vt_cross)

        ab2 = prep(base[0], vt_own, m_own, wt_half[1])
        ab2 = prep(base[2], vt_part, m_part, wt_half[1], ab2)
        ab2 = prep(base[1], vt_cross, m_cross, wt_half[1], ab2)
        a2, b2 = prep(base[3], vt_diag, m_diag, wt_half[1], ab2)
        t2, = products(tri_in_body, (), a2, b2, 2, 1, 7.2e9)

        dk_own, ds_own, dg2_own, pair_out, gwo2, gq2g, gq2s = head(0, t2, vt_own, gt_own, wgt[1], lnq[1], wot[1], wo[1], yt_own, True)
        dk_part = d2d(ds_own)
        dk_cross, ds_cross, dg2_cross = head(1, t2, vt_cross, gt_cross, wgt[1], lnq[1], wot[1], wo[1])
        dk_diag = d2d(ds_cross)
        da2, db2 = products(tri_in_bwd_body, (dk_own, dk_cross, dk_part, dk_diag), a2, b2, 2, 1, 14.4e9)
        et_own, gw2, gp2g, gp2s = back(0, da2, db2, yt_own, gt_own, dg2_own, m_own, ln[1], wt[1], wb[1], True, False)
        et_cross, = back(1, da2, db2, yt_cross, gt_cross, dg2_cross, m_cross, ln[1], wt[1], wb[1], False, False)

        dk_own, ds_own, dg1_own, gwo1, gq1g, gq1s = head(0, t1, xt_own, et_own, wgt[0], lnq[0], wot[0], wo[0], None, True)
        dk_part = d2d(ds_own)
        dk_cross, ds_cross, _ = head(1, t1, xt_cross, et_cross, wgt[0], lnq[0], wot[0], wo[0])
        dk_diag = d2d(ds_cross)
        da1, db1 = products(tri_out_bwd_body, (dk_own, dk_cross, dk_part, dk_diag), a1, b1, 1, 2, 7.2e9)
        d_pair, gw1, gp1g, gp1s = back(0, da1, db1, zt_own, et_own, dg1_own, m_own, ln[0], wt[0], wb[0], True, True)

        def vec(gg, gs):
            return jnp.stack([jnp.sum(gg, axis=1), jnp.sum(gs, axis=1)])

        def total(*parts):
            for swap in (d2d, ici):
                parts = tuple(v + swap(v) for v in parts)
            return parts

        def sums(gw, gpg, gps, gqg, gqs, gwo):
            vecs = jnp.concatenate([vec(gpg, gps), local(vec(gqg, gqs), 1)], axis=0)
            gw, gwo, vecs = total(gw, local(gwo, 0), jnp.concatenate([vecs, jnp.zeros_like(vecs)], axis=0))
            return vecs[0:2], proj_local(gw), gw[4 * C:].T, vecs[2:4], gwo

        def proj_local(g):
            return g[:4 * C].T

        def common(g):
            return jnp.concatenate([local(g[:4 * C].reshape(4, C, C), 1).reshape(4 * C, C), g[4 * C:]], axis=0)

        s2 = sums(common(gw2), gp2g, gp2s, gq2g, gq2s, gwo2)
        s1 = sums(common(gw1), gp1g, gp1s, gq1g, gq1s, gwo1)
        return (pair_out, d_pair) + tuple(jnp.stack([p, q]).astype(BF16) for p, q in zip(s1, s2))


    return jax.shard_map(device_step, mesh=mesh, in_specs=(row_spec, mask_spec, row_spec, full_spec, full_spec, full_spec, full_spec, full_spec), out_specs=(row_spec, row_spec, grad_spec, grad_spec, grad_spec, grad_spec, grad_spec), check_vma=False)
```

```python
import functools
import jax
import jax.numpy as jnp
from jax import lax
from jax.experimental import pallas as pl
from jax.experimental.pallas import tpu as pltpu
from jax.sharding import PartitionSpec as P

LN_EPS = 1e-5
AX = 'dap'
N = 384
C = 128
H = 64
TI = 16
RB = 96
CB = 8
NCH = 2
HC = H // NCH
UNROLL = 2
G = 2
ZC = 3
ZR = RB // ZC
F32 = jnp.float32
BF16 = jnp.bfloat16
ICI_SWAP = [(0, 2), (2, 0), (1, 3), (3, 1)]
D2D_SWAP = [(0, 1), (1, 0), (2, 3), (3, 2)]
OWN, CROSS, PART, DIAG = 0, 2, 1, 3


def dot(a, b, ca=1, cb=0):
    return lax.dot_general(a, b, (((ca,), (cb,)), ((), ())), preferred_element_type=F32)


def hat(v):
    mean = jnp.sum(v, axis=0, keepdims=True) * (1.0 / C)
    cen = v - mean
    var = jnp.sum(cen * cen, axis=0, keepdims=True) * (1.0 / C)
    rstd = lax.rsqrt(var + LN_EPS)
    return cen * rstd, rstd


def affine(h, ln_ref):
    return (h * ln_ref[:, 0:1] + ln_ref[:, 1:2]).astype(BF16)


def rows_loop(fn, unroll=UNROLL, n=TI // G):
    def step(i, carry):
        fn(i)
        return carry

    lax.fori_loop(0, n, step, 0, unroll=unroll)


def get(ref, i):
    return jnp.concatenate([ref[G * i + r] for r in range(G)], axis=1)


def put(ref, i, v):
    for r in range(G):
        ref[G * i + r] = v[:, r * N:(r + 1) * N]


def put_turned(ref, i, v):
    for r in range(G):
        ref[G * i + r] = v[:, r * N:(r + 1) * N].T


def get_mask(ref, i):
    return jnp.concatenate([ref[pl.ds(G * i + r, 1), :] for r in range(G)], axis=1).astype(BF16)


def fold(v):
    return functools.reduce(lambda p, q: p + q, [v[:, k * 128:(k + 1) * 128] for k in range(G * N // 128)])


def fill(scr, refs):
    at = 0
    for ref in refs:
        def move(k, ref=ref, at=at):
            c = pl.multiple_of(k * 16, 16)
            scr[:, pl.ds(at + c, 16), :] = jnp.swapaxes(ref[pl.ds(c, 16)], 0, 1)

        rows_loop(move, 1, ref.shape[0] // 16)
        at += ref.shape[0]


def flush(scr, refs):
    at = 0
    for ref in refs:
        def move(k, ref=ref, at=at):
            c = pl.multiple_of(k * 16, 16)
            ref[pl.ds(c, 16)] = jnp.swapaxes(scr[:, pl.ds(at + c, 16), :], 0, 1)

        rows_loop(move, 1, ref.shape[0] // 16)
        at += ref.shape[0]


def scr(n):
    return pltpu.VMEM((TI, n, N), BF16)


def const_spec(shape):
    nd = len(shape)
    return pl.BlockSpec(shape, lambda *_: (0,) * nd)


def act_spec():
    return pl.BlockSpec((TI, N, C), lambda i, *_: (i, 0, 0))


def actt_spec():
    return pl.BlockSpec((TI, C, N), lambda i, *_: (i, 0, 0))


def mask_spec_():
    return pl.BlockSpec((TI, N), lambda i, *_: (i, 0))


def piece_spec(k, n):
    return pl.BlockSpec((None, n, TI, N), lambda i: (k, 0, i, 0))


def half_spec():
    return pl.BlockSpec((H, TI, N), lambda i: (0, i, 0))


ACT = jax.ShapeDtypeStruct((RB, N, C), BF16)
ACTT = jax.ShapeDtypeStruct((RB, C, N), BF16)
HALF = jax.ShapeDtypeStruct((H, RB, N), BF16)
NPOS = RB * N


def cost(flops, nbytes, trans=0):
    return pl.CostEstimate(flops=int(flops), bytes_accessed=int(nbytes), transcendentals=int(trans))


def turn_body(z_ref, zt_ref):
    rows_loop(lambda i: put(zt_ref, i, jnp.concatenate([z_ref[G * i + r].T for r in range(G)], axis=1)))


def turn(z):
    return pl.pallas_call(turn_body, grid=(RB // TI,), in_specs=[act_spec()], out_specs=actt_spec(), out_shape=ACTT,
                          cost_estimate=cost(NPOS * C * 40, NPOS * C * 4), name="turn")(z)


def norm_body(z_ref, ln_ref, *rest):
    zt_ref, xt_ref, xc_ref = rest[-3:]

    def row(i):
        zt = jnp.concatenate([z_ref[G * i + r].T for r in range(G)], axis=1)
        put(zt_ref, i, zt)
        h, _ = hat(zt.astype(F32))
        x = affine(h, ln_ref)
        put(xt_ref, i, x)
        put(xc_ref, i, x)

    rows_loop(row)


def norm(z, ln, part=0, full=None):
    rows = z.shape[0]
    off = part * (ZR // TI)
    extra = () if full is None else tuple(full)
    spec = pl.BlockSpec((TI, C, N), lambda i: (i + off, 0, 0))
    return pl.pallas_call(norm_body, grid=(rows // TI,), in_specs=[act_spec(), const_spec((C, 2))] + [pl.BlockSpec(memory_space=pl.ANY)] * len(extra),
                          out_specs=[spec, spec, actt_spec()], out_shape=[ACTT, ACTT, jax.ShapeDtypeStruct((rows, C, N), BF16)],
                          input_output_aliases={2: 0, 3: 1} if extra else {},
                          cost_estimate=cost(rows * N * C * 60, rows * N * C * 8), name="norm")(z, ln, *extra)


def prep_body(base, x_ref, m_ref, wt_ref, *rest):
    a_out, b_out, sa, sb = rest[-4:]

    def row(i):
        p = dot(wt_ref[...], get(x_ref, i) * get_mask(m_ref, i))
        for out, at in ((sa, 0), (sb, 2 * H)):
            lin = p[at:at + H]
            put(out, i, (lin * jnp.tanh(p[at + H:at + 2 * H]) + lin).astype(BF16))

    rows_loop(row)
    flush(sa, [a_out])
    flush(sb, [b_out])


def prep(base, xt, mask, wt, full=None):
    rows = xt.shape[0]
    npos = rows * N
    out = jax.ShapeDtypeStruct((H, N, N), BF16)
    spec = pl.BlockSpec((H, TI, N), lambda i, b: (0, b[0] + i, 0))
    extra = () if full is None else tuple(full)
    grid_spec = pltpu.PrefetchScalarGridSpec(
        num_scalar_prefetch=1, grid=(rows // TI,),
        in_specs=[actt_spec(), mask_spec_(), const_spec((4 * H, C))] + [pl.BlockSpec(memory_space=pl.ANY)] * len(extra),
        out_specs=[spec, spec], scratch_shapes=[scr(H), scr(H)])
    return pl.pallas_call(
        prep_body, grid_spec=grid_spec, out_shape=[out, out],
        input_output_aliases={4: 0, 5: 1} if extra else {},
        cost_estimate=cost(npos * C * 400, npos * C * 4, npos * C), name="prep",
    )(base, xt, mask, wt, *extra)


def block_rows(idx, ref, c):
    return [ref[c, pl.ds(pl.multiple_of(idx[k] * RB, RB), RB), :] for k in range(4)]


def emit(vals, keep, send, c):
    keep[0, c] = vals[:RB]
    keep[1, c] = vals[RB:2 * RB]
    send[0, c] = vals[2 * RB:3 * RB]
    send[1, c] = vals[3 * RB:]


def tri_out_body(idx, a, b, keep, send):
    def chan(c):
        lhs = jnp.concatenate(block_rows(idx, a, c), axis=0)
        emit(dot(lhs, b[c], 1, 1).astype(BF16), keep, send, c)

    rows_loop(chan, 2, CB)


def tri_in_body(idx, a, b, keep, send, s):
    def chan(c):
        s[c] = a[c].T
        lhs = jnp.concatenate(block_rows(idx, s, c), axis=0)
        emit(dot(lhs, b[c]).astype(BF16), keep, send, c)

    rows_loop(chan, 2, CB)


def gather_dt(idx, parts, c, s):
    for k, part in enumerate(parts):
        s[c, pl.ds(pl.multiple_of(idx[k] * RB, RB), RB), :] = part[c]


def tri_in_bwd_body(idx, d0, d1, d2, d3, a, b, dak, das, dbk, dbs, s):
    def chan(c):
        gather_dt(idx, (d0, d1, d2, d3), c, s)
        emit(dot(jnp.concatenate(block_rows(idx, b, c), axis=0), s[c], 1, 1).astype(BF16), dak, das, c)
        emit(dot(jnp.concatenate(block_rows(idx, a, c), axis=0), s[c]).astype(BF16), dbk, dbs, c)

    rows_loop(chan, 2, CB)


def tri_out_bwd_body(idx, d0, d1, d2, d3, a, b, dak, das, dbk, dbs, s, st):
    def chan(c):
        gather_dt(idx, (d0, d1, d2, d3), c, s)
        da = dot(jnp.concatenate([d0[c], d2[c]], axis=0), b[c]).astype(BF16)
        st[c] = s[c].T
        rows = block_rows(idx, st, c)
        db = dot(jnp.concatenate([rows[0], rows[2]], axis=0), a[c]).astype(BF16)
        dak[0, c] = da[:RB]
        das[0, c] = da[RB:]
        dbk[0, c] = db[:RB]
        dbs[0, c] = db[RB:]

    rows_loop(chan, 2, CB)


def tri_call(body, idx, part, dts, ab, pieces, n_out, n_scr, flops):
    off = part * (HC // CB)
    dspec = pl.BlockSpec((CB, RB, N), lambda c, _: (c + off, 0, 0))
    fspec = pl.BlockSpec((CB, N, N), lambda c, _: (c + off, 0, 0))
    ospec = pl.BlockSpec((pieces, CB, RB, N), lambda c, _: (0, c, 0, 0))
    grid_spec = pltpu.PrefetchScalarGridSpec(
        num_scalar_prefetch=1, grid=(HC // CB,), in_specs=[dspec] * len(dts) + [fspec] * len(ab),
        out_specs=[ospec] * n_out, scratch_shapes=[pltpu.VMEM((CB, N, N), BF16)] * n_scr)
    return pl.pallas_call(body, grid_spec=grid_spec, out_shape=[jax.ShapeDtypeStruct((pieces, HC, RB, N), BF16)] * n_out,
                          cost_estimate=cost(flops, 50e6))(idx, *dts, *ab)


def finish_body(*refs):
    ts = refs[:2 * NCH]
    z_ref, x_ref, wg_ref, lnq_ref, wo_ref, ln_ref, z_out, x_out, st = refs[2 * NCH:]
    fill(st, ts)

    def row(i):
        th, _ = hat(get(st, i).astype(F32))
        upd = dot(wo_ref[...], affine(th, lnq_ref))
        gate = jnp.tanh(dot(wg_ref[...], get(x_ref, i)))
        zn = (get(z_ref, i).astype(F32) + (gate * upd + upd)).astype(BF16)
        put(z_out, i, zn)
        h, _ = hat(zn.astype(F32))
        put(x_out, i, affine(h, ln_ref))

    rows_loop(row)


def finish(k, ts, zt, xt, wgt, lnq, wot, ln_next):
    return pl.pallas_call(
        finish_body, grid=(RB // TI,),
        in_specs=[piece_spec(k, HC)] * (2 * NCH) + [actt_spec(), actt_spec(), const_spec((C, C)), const_spec((C, 2)), const_spec((C, C)), const_spec((C, 2))],
        out_specs=[actt_spec()] * 2, out_shape=[ACTT] * 2, scratch_shapes=[scr(C)],
        cost_estimate=cost(NPOS * C * 600, NPOS * C * 10, NPOS * C), name="finish",
    )(*ts, zt, xt, wgt, lnq, wot, ln_next)


def head_body(emit_z, emit_w, emit_dg, *refs):
    ts = refs[:2 * NCH]
    refs = list(refs[2 * NCH:])
    x_ref, g_ref, wg_ref, lnq_ref, wot_ref, wo_ref = refs[:6]
    k = 6
    if emit_z:
        z_ref = refs[k]
        k += 1
    dt_keep, dt_send = refs[k:k + 2]
    k += 2
    if emit_dg:
        dg_out = refs[k]
        k += 1
    if emit_z:
        z_out = refs[k]
        k += 1
    if emit_w:
        gwo, ggain, gshift = refs[k:k + 3]

        @pl.when(pl.program_id(0) == 0)
        def _():
            gwo[...] = jnp.zeros_like(gwo)
            ggain[...] = jnp.zeros_like(ggain)
            gshift[...] = jnp.zeros_like(gshift)

    st, sd = refs[-2:]
    fill(st, ts)

    def row(i):
        th, rstd = hat(get(st, i).astype(F32))
        if emit_dg:
            y = affine(th, lnq_ref)
            upd = dot(wot_ref[...], y)
        gate = jnp.tanh(dot(wg_ref[...], get(x_ref, i)))
        if emit_z:
            put_turned(z_out, i, (get(z_ref, i).astype(F32) + (gate * upd + upd)).astype(BF16))
        dgate = get(g_ref, i).astype(F32) * (0.5 * gate + 0.5)
        if emit_dg:
            put(dg_out, i, (dgate * (upd - upd * gate)).astype(BF16))
        du = dgate.astype(BF16)
        dy = dot(wo_ref[...], du).astype(BF16).astype(F32)
        dh = dy * lnq_ref[:, 0:1]
        m1 = jnp.sum(dh, axis=0, keepdims=True) * (1.0 / C)
        m2 = jnp.sum(dh * th, axis=0, keepdims=True) * (1.0 / C)
        put(sd, i, (rstd * (dh - m1 - th * m2)).astype(BF16))
        if emit_w:
            gwo[...] += dot(y, du, 1, 1)
            ggain[...] += fold(dy * th)
            gshift[...] += fold(dy)

    rows_loop(row)
    flush(sd, [dt_keep, dt_send])


def head(k, ts, xt, gt, wgt, lnq, wot, wo, zt=None, emit_w=False, emit_dg=True):
    emit_z = zt is not None
    in_specs = [piece_spec(k, HC)] * (2 * NCH) + [actt_spec(), actt_spec(), const_spec((C, C)), const_spec((C, 2)), const_spec((C, C)), const_spec((C, C))]
    out_shape = [HALF, HALF] + [ACTT] * emit_dg
    out_specs = [half_spec(), half_spec()] + [actt_spec()] * emit_dg
    extra = ()
    if emit_z:
        in_specs.append(actt_spec())
        extra = (zt,)
        out_shape.append(ACT)
        out_specs.append(act_spec())
    if emit_w:
        for s in ((C, C), (C, C), (C, C)):
            out_shape.append(jax.ShapeDtypeStruct(s, F32))
            out_specs.append(const_spec(s))
    return pl.pallas_call(
        functools.partial(head_body, emit_z, emit_w, emit_dg), grid=(RB // TI,), in_specs=in_specs,
        out_specs=out_specs, out_shape=out_shape, scratch_shapes=[scr(C), scr(C)],
        cost_estimate=cost(NPOS * C * 800, NPOS * C * 10, NPOS * C), name="head",
    )(*ts, xt, gt, wgt, lnq, wot, wo, *extra)


def back_body(n_ab, emit_w, last, *refs):
    das, dbs = refs[:n_ab], refs[n_ab:2 * n_ab]
    refs = refs[2 * n_ab:]
    z_ref, g_ref, dg_ref, m_ref, ln_ref, wt_ref, wb_ref, d_out = refs[:8]
    if emit_w:
        gw, ggain, gshift = refs[8:11]

        @pl.when(pl.program_id(0) == 0)
        def _():
            gw[...] = jnp.zeros_like(gw)
            ggain[...] = jnp.zeros_like(ggain)
            gshift[...] = jnp.zeros_like(gshift)

    sa, sb = refs[-2:]
    fill(sa, das)
    fill(sb, dbs)

    def row(i):
        xh, rstd = hat(get(z_ref, i).astype(F32))
        x = affine(xh, ln_ref)
        mrow = get_mask(m_ref, i)
        ds = []
        for s, at in ((sa, 0), (sb, 2 * C)):
            p = dot(wt_ref[at:at + 2 * C], x)
            th = jnp.tanh(p[C:])
            t0 = (get(s, i) * mrow).astype(F32) * (0.5 * th + 0.5)
            ds.append(t0.astype(BF16))
            ds.append((t0 * (p[:C] - p[:C] * th)).astype(BF16))
        dp = jnp.concatenate(ds + [get(dg_ref, i)], axis=0)
        dx = dot(wb_ref[...], dp).astype(BF16).astype(F32)
        dh = dx * ln_ref[:, 0:1]
        m1 = jnp.sum(dh, axis=0, keepdims=True) * (1.0 / C)
        m2 = jnp.sum(dh * xh, axis=0, keepdims=True) * (1.0 / C)
        d = (get(g_ref, i).astype(F32) + rstd * (dh - m1 - xh * m2)).astype(BF16)
        (put_turned if last else put)(d_out, i, d)
        if emit_w:
            gw[...] += dot(dp, x, 1, 1)
            ggain[...] += fold(dx * xh)
            gshift[...] += fold(dx)

    rows_loop(row)


def back(k, das, dbs, zt, gt, dgt, mask, ln, wt, wb, emit_w, last):
    n = len(das)
    out_shape = [ACT if last else ACTT]
    out_specs = [act_spec() if last else actt_spec()]
    if emit_w:
        for s in ((5 * C, C), (C, C), (C, C)):
            out_shape.append(jax.ShapeDtypeStruct(s, F32))
            out_specs.append(const_spec(s))
    return pl.pallas_call(
        functools.partial(back_body, n, emit_w, last), grid=(RB // TI,),
        in_specs=[piece_spec(k, HC)] * (2 * n) + [actt_spec()] * 3 + [mask_spec_(), const_spec((C, 2)), const_spec((4 * C, C)), const_spec((C, 5 * C))],
        out_specs=out_specs, out_shape=out_shape, scratch_shapes=[scr(C), scr(C)],
        cost_estimate=cost(NPOS * C * 2000, NPOS * C * 12, NPOS * C * 2), name="back",
    )(*das, *dbs, zt, gt, dgt, mask, ln, wt, wb)


def solution(mesh):
    row_spec = P(('data', 'dap'), None, None)
    mask_spec = P(('data', 'dap'), None)
    full_spec = P()
    grad_spec = P('data', None, None)

    def ici(v):
        return lax.ppermute(v, AX, ICI_SWAP)

    def d2d(v):
        return lax.ppermute(v, AX, D2D_SWAP)

    def device_step(pair_act, pair_mask, d_pair_out, ln_pair, w_proj, w_gate, ln_chan, w_out):
        me = lax.axis_index(AX)
        odd = (me & 1) == 1
        blocks = jnp.stack([me ^ OWN, me ^ CROSS, me ^ PART, me ^ DIAG]).astype(jnp.int32)
        base = [blocks[k:k + 1] * (RB // TI) for k in range(4)]

        def local(v, axis):
            return jnp.where(odd, jnp.roll(v, H, axis=axis), v)

        m_own = pair_mask.astype(F32)
        m_cross = ici(m_own)
        m_part = d2d(m_own)
        m_diag = d2d(m_cross)

        ln = [ln_pair[u].T.astype(F32) for u in range(2)]
        lnq = [local(ln_chan[u].T.astype(F32), 0) for u in range(2)]
        wp4 = [local(w_proj[u].reshape(C, 4, C), 2) for u in range(2)]
        wt_half = [(0.5 * wp4[u][:, :, :H]).reshape(C, 4 * H).T for u in range(2)]
        wt = [(0.5 * wp4[u]).reshape(C, 4 * C).T for u in range(2)]
        wb = [jnp.concatenate([wp4[u].reshape(C, 4 * C), w_gate[u]], axis=1) for u in range(2)]
        wgt = [0.5 * w_gate[u].T for u in range(2)]
        wo = [local(w_out[u], 0) for u in range(2)]
        wot = [0.5 * wo[u].T for u in range(2)]

        def products(body, dts, a, b, pieces, n_scr, flops):
            n_out = 4 if dts else 2
            res, sent = [], []
            for part in range(NCH):
                res.append(tri_call(body, blocks, part, dts, (a, b), pieces, n_out, n_scr, flops / NCH))
                sent.append([d2d(res[-1][j]) for j in range(1, n_out, 2)])
            keeps = [[r[j] for r in res] for j in range(0, n_out, 2)]
            sends = [list(v) for v in zip(*sent)]
            return [k + s for k, s in zip(keeps, sends)]

        z_parts = []
        for j in range(ZC):
            z_parts.append(ici(pair_act[j * ZR:(j + 1) * ZR]))
        zt_own, xt_own, _ = norm(pair_act, ln[0])
        xt_part = d2d(xt_own)
        gt_own = turn(d_pair_out)
        gt_cross = ici(gt_own)
        ab1 = prep(base[0], xt_own, m_own, wt_half[0])
        ab1 = prep(base[2], xt_part, m_part, wt_half[0], ab1)
        full = None
        for j in range(ZC):
            zt_cross, xt_cross, xc = norm(z_parts[j], ln[0], j, full)
            full = (zt_cross, xt_cross)
            xd = d2d(xc)
            rows = slice(j * ZR, (j + 1) * ZR)
            ab1 = prep(base[1] + j * (ZR // TI), xc, m_cross[rows], wt_half[0], ab1)
            ab1 = prep(base[3] + j * (ZR // TI), xd, m_diag[rows], wt_half[0], ab1)
        a1, b1 = ab1
        t1, = products(tri_out_body, (), a1, b1, 2, 0, 7.2e9)
        yt_own, vt_own = finish(0, t1, zt_own, xt_own, wgt[0], lnq[0], wot[0], ln[1])
        vt_part = d2d(vt_own)
        yt_cross, vt_cross = finish(1, t1, zt_cross, xt_cross, wgt[0], lnq[0], wot[0], ln[1])
        vt_diag = d2d(vt_cross)

        ab2 = prep(base[0], vt_own, m_own, wt_half[1])
        ab2 = prep(base[2], vt_part, m_part, wt_half[1], ab2)
        ab2 = prep(base[1], vt_cross, m_cross, wt_half[1], ab2)
        a2, b2 = prep(base[3], vt_diag, m_diag, wt_half[1], ab2)
        t2, = products(tri_in_body, (), a2, b2, 2, 1, 7.2e9)

        dk_own, ds_own, dg2_own, pair_out, gwo2, gq2g, gq2s = head(0, t2, vt_own, gt_own, wgt[1], lnq[1], wot[1], wo[1], yt_own, True)
        dk_part = d2d(ds_own)
        dk_cross, ds_cross, dg2_cross = head(1, t2, vt_cross, gt_cross, wgt[1], lnq[1], wot[1], wo[1])
        dk_diag = d2d(ds_cross)
        da2, db2 = products(tri_in_bwd_body, (dk_own, dk_cross, dk_part, dk_diag), a2, b2, 2, 1, 14.4e9)
        et_own, gw2, gp2g, gp2s = back(0, da2, db2, yt_own, gt_own, dg2_own, m_own, ln[1], wt[1], wb[1], True, False)
        et_cross, = back(1, da2, db2, yt_cross, gt_cross, dg2_cross, m_cross, ln[1], wt[1], wb[1], False, False)

        dk_own, ds_own, dg1_own, gwo1, gq1g, gq1s = head(0, t1, xt_own, et_own, wgt[0], lnq[0], wot[0], wo[0], None, True)
        dk_part = d2d(ds_own)

        def vec(gg, gs):
            return jnp.stack([jnp.sum(gg, axis=1), jnp.sum(gs, axis=1)])

        def common(g):
            return jnp.concatenate([local(g[:4 * C].reshape(4, C, C), 1).reshape(4 * C, C), g[4 * C:]], axis=0)

        def total(v):
            w = d2d(v)
            v = v + w
            w = ici(v)
            return v + w

        early = total(jnp.concatenate([common(gw2), local(gwo2, 0), local(gwo1, 0), vec(gp2g, gp2s),
                                       local(vec(gq2g, gq2s), 1), local(vec(gq1g, gq1s), 1), jnp.zeros((2, C), F32)], axis=0))
        dk_cross, ds_cross = head(1, t1, xt_cross, et_cross, wgt[0], lnq[0], wot[0], wo[0], None, False, False)
        dk_diag = d2d(ds_cross)
        da1, db1 = products(tri_out_bwd_body, (dk_own, dk_cross, dk_part, dk_diag), a1, b1, 1, 2, 7.2e9)
        d_pair, gw1, gp1g, gp1s = back(0, da1, db1, zt_own, et_own, dg1_own, m_own, ln[0], wt[0], wb[0], True, True)
        late = total(jnp.concatenate([common(gw1), vec(gp1g, gp1s), jnp.zeros((6, C), F32)], axis=0))
        e0, e1, e2 = 5 * C, 6 * C, 7 * C
        grads = (jnp.stack([late[e0:e0 + 2], early[e2:e2 + 2]]),
                 jnp.stack([late[:4 * C].T, early[:4 * C].T]),
                 jnp.stack([late[4 * C:e0].T, early[4 * C:e0].T]),
                 jnp.stack([early[e2 + 4:e2 + 6], early[e2 + 2:e2 + 4]]),
                 jnp.stack([early[e1:e2], early[e0:e1]]))
        return (pair_out, d_pair) + tuple(v.astype(BF16) for v in grads)


    return jax.shard_map(device_step, mesh=mesh, in_specs=(row_spec, mask_spec, row_spec, full_spec, full_spec, full_spec, full_spec, full_spec), out_specs=(row_spec, row_spec, grad_spec, grad_spec, grad_spec, grad_spec, grad_spec), check_vma=False)
```

```python
import functools
import jax
import jax.numpy as jnp
from jax import lax
from jax.experimental import pallas as pl
from jax.experimental.pallas import tpu as pltpu
from jax.sharding import PartitionSpec as P

LN_EPS = 1e-5
AX = 'dap'
N = 384
C = 128
H = 64
TI = 16
RB = 96
CB = 8
NCH = 2
HC = H // NCH
UNROLL = 2
G = 2
ZC = 6
BACK_UNROLL = 4
ZR = RB // ZC
F32 = jnp.float32
BF16 = jnp.bfloat16
ICI_SWAP = [(0, 2), (2, 0), (1, 3), (3, 1)]
D2D_SWAP = [(0, 1), (1, 0), (2, 3), (3, 2)]
OWN, CROSS, PART, DIAG = 0, 2, 1, 3


def dot(a, b, ca=1, cb=0):
    return lax.dot_general(a, b, (((ca,), (cb,)), ((), ())), preferred_element_type=F32)


def hat(v):
    mean = jnp.sum(v, axis=0, keepdims=True) * (1.0 / C)
    cen = v - mean
    var = jnp.sum(cen * cen, axis=0, keepdims=True) * (1.0 / C)
    rstd = lax.rsqrt(var + LN_EPS)
    return cen * rstd, rstd


def affine(h, ln_ref):
    return (h * ln_ref[:, 0:1] + ln_ref[:, 1:2]).astype(BF16)


def rows_loop(fn, unroll=UNROLL, n=TI // G):
    def step(i, carry):
        fn(i)
        return carry

    lax.fori_loop(0, n, step, 0, unroll=unroll)


def get(ref, i):
    return jnp.concatenate([ref[G * i + r] for r in range(G)], axis=1)


def put(ref, i, v):
    for r in range(G):
        ref[G * i + r] = v[:, r * N:(r + 1) * N]


def put_turned(ref, i, v):
    for r in range(G):
        ref[G * i + r] = v[:, r * N:(r + 1) * N].T


def get_mask(ref, i):
    return jnp.concatenate([ref[pl.ds(G * i + r, 1), :] for r in range(G)], axis=1).astype(BF16)


def fold(v):
    return functools.reduce(lambda p, q: p + q, [v[:, k * 128:(k + 1) * 128] for k in range(G * N // 128)])


def fill(scr, refs):
    at = 0
    for ref in refs:
        def move(k, ref=ref, at=at):
            c = pl.multiple_of(k * 16, 16)
            scr[:, pl.ds(at + c, 16), :] = jnp.swapaxes(ref[pl.ds(c, 16)], 0, 1)

        rows_loop(move, 1, ref.shape[0] // 16)
        at += ref.shape[0]


def flush(scr, refs):
    at = 0
    for ref in refs:
        def move(k, ref=ref, at=at):
            c = pl.multiple_of(k * 16, 16)
            ref[pl.ds(c, 16)] = jnp.swapaxes(scr[:, pl.ds(at + c, 16), :], 0, 1)

        rows_loop(move, 1, ref.shape[0] // 16)
        at += ref.shape[0]


def scr(n):
    return pltpu.VMEM((TI, n, N), BF16)


def const_spec(shape):
    nd = len(shape)
    return pl.BlockSpec(shape, lambda *_: (0,) * nd)


def act_spec():
    return pl.BlockSpec((TI, N, C), lambda i, *_: (i, 0, 0))


def actt_spec():
    return pl.BlockSpec((TI, C, N), lambda i, *_: (i, 0, 0))


def mask_spec_():
    return pl.BlockSpec((TI, N), lambda i, *_: (i, 0))


def piece_spec(k, n):
    return pl.BlockSpec((None, n, TI, N), lambda i: (k, 0, i, 0))


def half_spec():
    return pl.BlockSpec((H, TI, N), lambda i: (0, i, 0))


ACT = jax.ShapeDtypeStruct((RB, N, C), BF16)
ACTT = jax.ShapeDtypeStruct((RB, C, N), BF16)
HALF = jax.ShapeDtypeStruct((H, RB, N), BF16)
NPOS = RB * N


def cost(flops, nbytes, trans=0):
    return pl.CostEstimate(flops=int(flops), bytes_accessed=int(nbytes), transcendentals=int(trans))


def turn_body(z_ref, zt_ref):
    rows_loop(lambda i: put(zt_ref, i, jnp.concatenate([z_ref[G * i + r].T for r in range(G)], axis=1)))


def turn(z):
    return pl.pallas_call(turn_body, grid=(RB // TI,), in_specs=[act_spec()], out_specs=actt_spec(), out_shape=ACTT,
                          cost_estimate=cost(NPOS * C * 40, NPOS * C * 4), name="turn")(z)


def norm_body(unroll, _, z_ref, ln_ref, *rest):
    zt_ref, xt_ref, xc_ref = rest[-3:]

    def row(i):
        zt = jnp.concatenate([z_ref[G * i + r].T for r in range(G)], axis=1)
        put(zt_ref, i, zt)
        h, _ = hat(zt.astype(F32))
        x = affine(h, ln_ref)
        put(xt_ref, i, x)
        put(xc_ref, i, x)

    rows_loop(row, unroll)


def norm(z, ln, part=0, full=None):
    rows = z.shape[0]
    extra = () if full is None else tuple(full)
    spec = pl.BlockSpec((TI, C, N), lambda i, p: (i + p[0], 0, 0))
    grid_spec = pltpu.PrefetchScalarGridSpec(
        num_scalar_prefetch=1, grid=(rows // TI,),
        in_specs=[act_spec(), const_spec((C, 2))] + [pl.BlockSpec(memory_space=pl.ANY)] * len(extra),
        out_specs=[spec, spec, actt_spec()])
    return pl.pallas_call(functools.partial(norm_body, UNROLL if rows == RB else 1), grid_spec=grid_spec, out_shape=[ACTT, ACTT, jax.ShapeDtypeStruct((rows, C, N), BF16)],
                          input_output_aliases={3: 0, 4: 1} if extra else {},
                          cost_estimate=cost(rows * N * C * 60, rows * N * C * 8), name="norm")(
        jnp.full((1,), part * (ZR // TI), jnp.int32), z, ln, *extra)


def prep_body(unroll, base, x_ref, m_ref, wt_ref, *rest):
    a_out, b_out, sa, sb = rest[-4:]

    def row(i):
        p = dot(wt_ref[...], get(x_ref, i) * get_mask(m_ref, i))
        for out, at in ((sa, 0), (sb, 2 * H)):
            lin = p[at:at + H]
            put(out, i, (lin * jnp.tanh(p[at + H:at + 2 * H]) + lin).astype(BF16))

    rows_loop(row, unroll)
    flush(sa, [a_out])
    flush(sb, [b_out])


def prep(base, xt, mask, wt, full=None):
    rows = xt.shape[0]
    npos = rows * N
    out = jax.ShapeDtypeStruct((H, N, N), BF16)
    spec = pl.BlockSpec((H, TI, N), lambda i, b: (0, b[0] + i, 0))
    extra = () if full is None else tuple(full)
    grid_spec = pltpu.PrefetchScalarGridSpec(
        num_scalar_prefetch=1, grid=(rows // TI,),
        in_specs=[actt_spec(), mask_spec_(), const_spec((4 * H, C))] + [pl.BlockSpec(memory_space=pl.ANY)] * len(extra),
        out_specs=[spec, spec], scratch_shapes=[scr(H), scr(H)])
    return pl.pallas_call(
        functools.partial(prep_body, UNROLL if rows == RB else 1), grid_spec=grid_spec, out_shape=[out, out],
        input_output_aliases={4: 0, 5: 1} if extra else {},
        cost_estimate=cost(npos * C * 400, npos * C * 4, npos * C), name="prep",
    )(base, xt, mask, wt, *extra)


def block_rows(idx, ref, c):
    return [ref[c, pl.ds(pl.multiple_of(idx[k] * RB, RB), RB), :] for k in range(4)]


def emit(vals, keep, send, c):
    keep[0, c] = vals[:RB]
    keep[1, c] = vals[RB:2 * RB]
    send[0, c] = vals[2 * RB:3 * RB]
    send[1, c] = vals[3 * RB:]


def tri_out_body(idx, a, b, keep, send):
    def chan(c):
        lhs = jnp.concatenate(block_rows(idx, a, c), axis=0)
        emit(dot(lhs, b[c], 1, 1).astype(BF16), keep, send, c)

    rows_loop(chan, 2, CB)


def tri_in_body(idx, a, b, keep, send, s):
    def chan(c):
        s[c] = a[c].T
        lhs = jnp.concatenate(block_rows(idx, s, c), axis=0)
        emit(dot(lhs, b[c]).astype(BF16), keep, send, c)

    rows_loop(chan, 2, CB)


def gather_dt(idx, parts, c, s):
    for k, part in enumerate(parts):
        s[c, pl.ds(pl.multiple_of(idx[k] * RB, RB), RB), :] = part[c]


def tri_in_bwd_body(idx, d0, d1, d2, d3, a, b, dak, das, dbk, dbs, s):
    def chan(c):
        gather_dt(idx, (d0, d1, d2, d3), c, s)
        emit(dot(jnp.concatenate(block_rows(idx, b, c), axis=0), s[c], 1, 1).astype(BF16), dak, das, c)
        emit(dot(jnp.concatenate(block_rows(idx, a, c), axis=0), s[c]).astype(BF16), dbk, dbs, c)

    rows_loop(chan, 2, CB)


def tri_out_bwd_body(idx, d0, d1, d2, d3, a, b, dak, das, dbk, dbs, s, st):
    def chan(c):
        gather_dt(idx, (d0, d1, d2, d3), c, s)
        da = dot(jnp.concatenate([d0[c], d2[c]], axis=0), b[c]).astype(BF16)
        st[c] = s[c].T
        rows = block_rows(idx, st, c)
        db = dot(jnp.concatenate([rows[0], rows[2]], axis=0), a[c]).astype(BF16)
        dak[0, c] = da[:RB]
        das[0, c] = da[RB:]
        dbk[0, c] = db[:RB]
        dbs[0, c] = db[RB:]

    rows_loop(chan, 2, CB)


def tri_call(body, idx, part, dts, ab, pieces, n_out, n_scr, flops):
    idx = jnp.concatenate([idx, jnp.full((1,), part * (HC // CB), jnp.int32)])
    dspec = pl.BlockSpec((CB, RB, N), lambda c, i: (c + i[4], 0, 0))
    fspec = pl.BlockSpec((CB, N, N), lambda c, i: (c + i[4], 0, 0))
    ospec = pl.BlockSpec((pieces, CB, RB, N), lambda c, _: (0, c, 0, 0))
    grid_spec = pltpu.PrefetchScalarGridSpec(
        num_scalar_prefetch=1, grid=(HC // CB,), in_specs=[dspec] * len(dts) + [fspec] * len(ab),
        out_specs=[ospec] * n_out, scratch_shapes=[pltpu.VMEM((CB, N, N), BF16)] * n_scr)
    return pl.pallas_call(body, grid_spec=grid_spec, out_shape=[jax.ShapeDtypeStruct((pieces, HC, RB, N), BF16)] * n_out,
                          cost_estimate=cost(flops, 50e6))(idx, *dts, *ab)


def finish_body(_, *refs):
    ts = refs[:2 * NCH]
    z_ref, x_ref, wg_ref, lnq_ref, wo_ref, ln_ref, z_out, x_out, st = refs[2 * NCH:]
    fill(st, ts)

    def row(i):
        th, _ = hat(get(st, i).astype(F32))
        upd = dot(wo_ref[...], affine(th, lnq_ref))
        gate = jnp.tanh(dot(wg_ref[...], get(x_ref, i)))
        zn = (get(z_ref, i).astype(F32) + (gate * upd + upd)).astype(BF16)
        put(z_out, i, zn)
        h, _ = hat(zn.astype(F32))
        put(x_out, i, affine(h, ln_ref))

    rows_loop(row)


def finish(k, ts, zt, xt, wgt, lnq, wot, ln_next):
    tspec = pl.BlockSpec((None, HC, TI, N), lambda i, p: (p[0], 0, i, 0))
    grid_spec = pltpu.PrefetchScalarGridSpec(
        num_scalar_prefetch=1, grid=(RB // TI,),
        in_specs=[tspec] * (2 * NCH) + [actt_spec(), actt_spec(), const_spec((C, C)), const_spec((C, 2)), const_spec((C, C)), const_spec((C, 2))],
        out_specs=[actt_spec()] * 2, scratch_shapes=[scr(C)])
    return pl.pallas_call(
        finish_body, grid_spec=grid_spec, out_shape=[ACTT] * 2,
        cost_estimate=cost(NPOS * C * 600, NPOS * C * 10, NPOS * C), name="finish",
    )(jnp.full((1,), k, jnp.int32), *ts, zt, xt, wgt, lnq, wot, ln_next)


def head_body(emit_z, emit_w, emit_dg, *refs):
    ts = refs[:2 * NCH]
    refs = list(refs[2 * NCH:])
    x_ref, g_ref, wg_ref, lnq_ref, wot_ref, wo_ref = refs[:6]
    k = 6
    if emit_z:
        z_ref = refs[k]
        k += 1
    dt_keep, dt_send = refs[k:k + 2]
    k += 2
    if emit_dg:
        dg_out = refs[k]
        k += 1
    if emit_z:
        z_out = refs[k]
        k += 1
    if emit_w:
        gwo, ggain, gshift = refs[k:k + 3]

        @pl.when(pl.program_id(0) == 0)
        def _():
            gwo[...] = jnp.zeros_like(gwo)
            ggain[...] = jnp.zeros_like(ggain)
            gshift[...] = jnp.zeros_like(gshift)

    st, sd = refs[-2:]
    fill(st, ts)

    def row(i):
        th, rstd = hat(get(st, i).astype(F32))
        if emit_dg:
            y = affine(th, lnq_ref)
            upd = dot(wot_ref[...], y)
        gate = jnp.tanh(dot(wg_ref[...], get(x_ref, i)))
        if emit_z:
            put_turned(z_out, i, (get(z_ref, i).astype(F32) + (gate * upd + upd)).astype(BF16))
        dgate = get(g_ref, i).astype(F32) * (0.5 * gate + 0.5)
        if emit_dg:
            put(dg_out, i, (dgate * (upd - upd * gate)).astype(BF16))
        du = dgate.astype(BF16)
        dy = dot(wo_ref[...], du).astype(BF16).astype(F32)
        dh = dy * lnq_ref[:, 0:1]
        m1 = jnp.sum(dh, axis=0, keepdims=True) * (1.0 / C)
        m2 = jnp.sum(dh * th, axis=0, keepdims=True) * (1.0 / C)
        put(sd, i, (rstd * (dh - m1 - th * m2)).astype(BF16))
        if emit_w:
            gwo[...] += dot(y, du, 1, 1)
            ggain[...] += fold(dy * th)
            gshift[...] += fold(dy)

    rows_loop(row)
    flush(sd, [dt_keep, dt_send])


def head(k, ts, xt, gt, wgt, lnq, wot, wo, zt=None, emit_w=False, emit_dg=True):
    emit_z = zt is not None
    in_specs = [piece_spec(k, HC)] * (2 * NCH) + [actt_spec(), actt_spec(), const_spec((C, C)), const_spec((C, 2)), const_spec((C, C)), const_spec((C, C))]
    out_shape = [HALF, HALF] + [ACTT] * emit_dg
    out_specs = [half_spec(), half_spec()] + [actt_spec()] * emit_dg
    extra = ()
    if emit_z:
        in_specs.append(actt_spec())
        extra = (zt,)
        out_shape.append(ACT)
        out_specs.append(act_spec())
    if emit_w:
        for s in ((C, C), (C, C), (C, C)):
            out_shape.append(jax.ShapeDtypeStruct(s, F32))
            out_specs.append(const_spec(s))
    return pl.pallas_call(
        functools.partial(head_body, emit_z, emit_w, emit_dg), grid=(RB // TI,), in_specs=in_specs,
        out_specs=out_specs, out_shape=out_shape, scratch_shapes=[scr(C), scr(C)],
        cost_estimate=cost(NPOS * C * 800, NPOS * C * 10, NPOS * C), name="head",
    )(*ts, xt, gt, wgt, lnq, wot, wo, *extra)


def back_body(n_ab, emit_w, last, *refs):
    das, dbs = refs[:n_ab], refs[n_ab:2 * n_ab]
    refs = refs[2 * n_ab:]
    z_ref, g_ref, dg_ref, m_ref, ln_ref, wt_ref, wb_ref, d_out = refs[:8]
    if emit_w:
        gw, ggain, gshift = refs[8:11]

        @pl.when(pl.program_id(0) == 0)
        def _():
            gw[...] = jnp.zeros_like(gw)
            ggain[...] = jnp.zeros_like(ggain)
            gshift[...] = jnp.zeros_like(gshift)

    sa, sb = refs[-2:]
    fill(sa, das)
    fill(sb, dbs)

    def row(i):
        xh, rstd = hat(get(z_ref, i).astype(F32))
        x = affine(xh, ln_ref)
        mrow = get_mask(m_ref, i)
        ds = []
        for s, at in ((sa, 0), (sb, 2 * C)):
            p = dot(wt_ref[at:at + 2 * C], x)
            th = jnp.tanh(p[C:])
            t0 = (get(s, i) * mrow).astype(F32) * (0.5 * th + 0.5)
            ds.append(t0.astype(BF16))
            ds.append((t0 * (p[:C] - p[:C] * th)).astype(BF16))
        dp = jnp.concatenate(ds + [get(dg_ref, i)], axis=0)
        dx = dot(wb_ref[...], dp).astype(BF16).astype(F32)
        dh = dx * ln_ref[:, 0:1]
        m1 = jnp.sum(dh, axis=0, keepdims=True) * (1.0 / C)
        m2 = jnp.sum(dh * xh, axis=0, keepdims=True) * (1.0 / C)
        d = (get(g_ref, i).astype(F32) + rstd * (dh - m1 - xh * m2)).astype(BF16)
        (put_turned if last else put)(d_out, i, d)
        if emit_w:
            gw[...] += dot(dp, x, 1, 1)
            ggain[...] += fold(dx * xh)
            gshift[...] += fold(dx)

    rows_loop(row, BACK_UNROLL if emit_w else UNROLL)


def back(k, das, dbs, zt, gt, dgt, mask, ln, wt, wb, emit_w, last):
    n = len(das)
    out_shape = [ACT if last else ACTT]
    out_specs = [act_spec() if last else actt_spec()]
    if emit_w:
        for s in ((5 * C, C), (C, C), (C, C)):
            out_shape.append(jax.ShapeDtypeStruct(s, F32))
            out_specs.append(const_spec(s))
    return pl.pallas_call(
        functools.partial(back_body, n, emit_w, last), grid=(RB // TI,),
        in_specs=[piece_spec(k, HC)] * (2 * n) + [actt_spec()] * 3 + [mask_spec_(), const_spec((C, 2)), const_spec((4 * C, C)), const_spec((C, 5 * C))],
        out_specs=out_specs, out_shape=out_shape, scratch_shapes=[scr(C), scr(C)],
        cost_estimate=cost(NPOS * C * 2000, NPOS * C * 12, NPOS * C * 2), name="back",
    )(*das, *dbs, zt, gt, dgt, mask, ln, wt, wb)


def solution(mesh):
    row_spec = P(('data', 'dap'), None, None)
    mask_spec = P(('data', 'dap'), None)
    full_spec = P()
    grad_spec = P('data', None, None)

    def ici(v):
        return lax.ppermute(v, AX, ICI_SWAP)

    def d2d(v):
        return lax.ppermute(v, AX, D2D_SWAP)

    def device_step(pair_act, pair_mask, d_pair_out, ln_pair, w_proj, w_gate, ln_chan, w_out):
        me = lax.axis_index(AX)
        odd = (me & 1) == 1
        blocks = jnp.stack([me ^ OWN, me ^ CROSS, me ^ PART, me ^ DIAG]).astype(jnp.int32)
        base = [blocks[k:k + 1] * (RB // TI) for k in range(4)]

        def local(v, axis):
            return jnp.where(odd, jnp.roll(v, H, axis=axis), v)

        m_own = pair_mask.astype(F32)
        m_cross = ici(m_own)
        m_part = d2d(m_own)
        m_diag = d2d(m_cross)

        ln = [ln_pair[u].T.astype(F32) for u in range(2)]
        lnq = [local(ln_chan[u].T.astype(F32), 0) for u in range(2)]
        wp4 = [local(w_proj[u].reshape(C, 4, C), 2) for u in range(2)]
        wt_half = [(0.5 * wp4[u][:, :, :H]).reshape(C, 4 * H).T for u in range(2)]
        wt = [(0.5 * wp4[u]).reshape(C, 4 * C).T for u in range(2)]
        wb = [jnp.concatenate([wp4[u].reshape(C, 4 * C), w_gate[u]], axis=1) for u in range(2)]
        wgt = [0.5 * w_gate[u].T for u in range(2)]
        wo = [local(w_out[u], 0) for u in range(2)]
        wot = [0.5 * wo[u].T for u in range(2)]

        def products(body, dts, a, b, pieces, n_scr, flops):
            n_out = 4 if dts else 2
            res, sent = [], []
            for part in range(NCH):
                res.append(tri_call(body, blocks, part, dts, (a, b), pieces, n_out, n_scr, flops / NCH))
                sent.append([d2d(res[-1][j]) for j in range(1, n_out, 2)])
            keeps = [[r[j] for r in res] for j in range(0, n_out, 2)]
            sends = [list(v) for v in zip(*sent)]
            return [k + s for k, s in zip(keeps, sends)]

        z_parts = []
        later = lax.optimization_barrier(pair_act)
        for j in range(ZC):
            z_parts.append(ici((later if j else pair_act)[j * ZR:(j + 1) * ZR]))
        zt_own, xt_own, _ = norm(pair_act, ln[0])
        xt_part = d2d(xt_own)
        gt_own = turn(d_pair_out)
        gt_cross = ici(gt_own)
        ab1 = prep(base[0], xt_own, m_own, wt_half[0])
        ab1 = prep(base[2], xt_part, m_part, wt_half[0], ab1)
        full = None
        for j in range(ZC):
            zt_cross, xt_cross, xc = norm(z_parts[j], ln[0], j, full)
            full = (zt_cross, xt_cross)
            xd = d2d(xc)
            rows = slice(j * ZR, (j + 1) * ZR)
            ab1 = prep(base[1] + j * (ZR // TI), xc, m_cross[rows], wt_half[0], ab1)
            ab1 = prep(base[3] + j * (ZR // TI), xd, m_diag[rows], wt_half[0], ab1)
        a1, b1 = ab1
        t1, = products(tri_out_body, (), a1, b1, 2, 0, 7.2e9)
        yt_own, vt_own = finish(0, t1, zt_own, xt_own, wgt[0], lnq[0], wot[0], ln[1])
        vt_part = d2d(vt_own)
        yt_cross, vt_cross = finish(1, t1, zt_cross, xt_cross, wgt[0], lnq[0], wot[0], ln[1])
        vt_diag = d2d(vt_cross)

        ab2 = prep(base[0], vt_own, m_own, wt_half[1])
        ab2 = prep(base[2], vt_part, m_part, wt_half[1], ab2)
        ab2 = prep(base[1], vt_cross, m_cross, wt_half[1], ab2)
        a2, b2 = prep(base[3], vt_diag, m_diag, wt_half[1], ab2)
        t2, = products(tri_in_body, (), a2, b2, 2, 1, 7.2e9)

        dk_own, ds_own, dg2_own, pair_out, gwo2, gq2g, gq2s = head(0, t2, vt_own, gt_own, wgt[1], lnq[1], wot[1], wo[1], yt_own, True)
        dk_part = d2d(ds_own)
        dk_cross, ds_cross, dg2_cross = head(1, t2, vt_cross, gt_cross, wgt[1], lnq[1], wot[1], wo[1])
        dk_diag = d2d(ds_cross)
        da2, db2 = products(tri_in_bwd_body, (dk_own, dk_cross, dk_part, dk_diag), a2, b2, 2, 1, 14.4e9)
        et_own, gw2, gp2g, gp2s = back(0, da2, db2, yt_own, gt_own, dg2_own, m_own, ln[1], wt[1], wb[1], True, False)
        et_cross, = back(1, da2, db2, yt_cross, gt_cross, dg2_cross, m_cross, ln[1], wt[1], wb[1], False, False)

        dk_own, ds_own, dg1_own, gwo1, gq1g, gq1s = head(0, t1, xt_own, et_own, wgt[0], lnq[0], wot[0], wo[0], None, True)
        dk_part = d2d(ds_own)

        def vec(gg, gs):
            return jnp.stack([jnp.sum(gg, axis=1), jnp.sum(gs, axis=1)])

        def common(g):
            return jnp.concatenate([local(g[:4 * C].reshape(4, C, C), 1).reshape(4 * C, C), g[4 * C:]], axis=0)

        def total(v):
            w = d2d(v)
            v = v + w
            w = ici(v)
            return v + w

        early = total(jnp.concatenate([common(gw2), local(gwo2, 0), local(gwo1, 0), vec(gp2g, gp2s),
                                       local(vec(gq2g, gq2s), 1), local(vec(gq1g, gq1s), 1), jnp.zeros((2, C), F32)], axis=0))
        dk_cross, ds_cross = head(1, t1, xt_cross, et_cross, wgt[0], lnq[0], wot[0], wo[0], None, False, False)
        dk_diag = d2d(ds_cross)
        da1, db1 = products(tri_out_bwd_body, (dk_own, dk_cross, dk_part, dk_diag), a1, b1, 1, 2, 7.2e9)
        d_pair, gw1, gp1g, gp1s = back(0, da1, db1, zt_own, et_own, dg1_own, m_own, ln[0], wt[0], wb[0], True, True)
        late = total(jnp.concatenate([common(gw1), vec(gp1g, gp1s), jnp.zeros((6, C), F32)], axis=0))
        e0, e1, e2 = 5 * C, 6 * C, 7 * C
        grads = (jnp.stack([late[e0:e0 + 2], early[e2:e2 + 2]]),
                 jnp.stack([late[:4 * C].T, early[:4 * C].T]),
                 jnp.stack([late[4 * C:e0].T, early[4 * C:e0].T]),
                 jnp.stack([early[e2 + 4:e2 + 6], early[e2 + 2:e2 + 4]]),
                 jnp.stack([early[e1:e2], early[e0:e1]]))
        return (pair_out, d_pair) + tuple(v.astype(BF16) for v in grads)


    return jax.shard_map(device_step, mesh=mesh, in_specs=(row_spec, mask_spec, row_spec, full_spec, full_spec, full_spec, full_spec, full_spec), out_specs=(row_spec, row_spec, grad_spec, grad_spec, grad_spec, grad_spec, grad_spec), check_vma=False)
```

```python
import functools
import jax
import jax.numpy as jnp
from jax import lax
from jax.experimental import pallas as pl
from jax.experimental.pallas import tpu as pltpu
from jax.sharding import PartitionSpec as P

LN_EPS = 1e-5
AX = 'dap'
N = 384
C = 128
H = 64
TI = 16
RB = 96
CB = 8
NCH = 2
HC = H // NCH
UNROLL = 2
G = 2
ZC = 6
BACK_UNROLL = 4
ZR = RB // ZC
F32 = jnp.float32
BF16 = jnp.bfloat16
ICI_SWAP = [(0, 2), (2, 0), (1, 3), (3, 1)]
D2D_SWAP = [(0, 1), (1, 0), (2, 3), (3, 2)]
OWN, CROSS, PART, DIAG = 0, 2, 1, 3


def dot(a, b, ca=1, cb=0):
    return lax.dot_general(a, b, (((ca,), (cb,)), ((), ())), preferred_element_type=F32)


def hat(v):
    mean = jnp.sum(v, axis=0, keepdims=True) * (1.0 / C)
    cen = v - mean
    var = jnp.sum(cen * cen, axis=0, keepdims=True) * (1.0 / C)
    rstd = lax.rsqrt(var + LN_EPS)
    return cen * rstd, rstd


def affine(h, ln_ref):
    return (h * ln_ref[:, 0:1] + ln_ref[:, 1:2]).astype(BF16)


def rows_loop(fn, unroll=UNROLL, n=TI // G):
    def step(i, carry):
        fn(i)
        return carry

    lax.fori_loop(0, n, step, 0, unroll=unroll)


def get(ref, i):
    return jnp.concatenate([ref[G * i + r] for r in range(G)], axis=1)


def put(ref, i, v):
    for r in range(G):
        ref[G * i + r] = v[:, r * N:(r + 1) * N]


def put_turned(ref, i, v):
    for r in range(G):
        ref[G * i + r] = v[:, r * N:(r + 1) * N].T


def get_mask(ref, i):
    return jnp.concatenate([ref[pl.ds(G * i + r, 1), :] for r in range(G)], axis=1).astype(BF16)


def fold(v):
    return functools.reduce(lambda p, q: p + q, [v[:, k * 128:(k + 1) * 128] for k in range(G * N // 128)])


def fill(scr, refs):
    at = 0
    for ref in refs:
        def move(k, ref=ref, at=at):
            c = pl.multiple_of(k * 16, 16)
            scr[:, pl.ds(at + c, 16), :] = jnp.swapaxes(ref[pl.ds(c, 16)], 0, 1)

        rows_loop(move, 1, ref.shape[0] // 16)
        at += ref.shape[0]


def flush(scr, refs):
    at = 0
    for ref in refs:
        def move(k, ref=ref, at=at):
            c = pl.multiple_of(k * 16, 16)
            ref[pl.ds(c, 16)] = jnp.swapaxes(scr[:, pl.ds(at + c, 16), :], 0, 1)

        rows_loop(move, 1, ref.shape[0] // 16)
        at += ref.shape[0]


def scr(n):
    return pltpu.VMEM((TI, n, N), BF16)


def const_spec(shape):
    nd = len(shape)
    return pl.BlockSpec(shape, lambda *_: (0,) * nd)


def act_spec():
    return pl.BlockSpec((TI, N, C), lambda i, *_: (i, 0, 0))


def actt_spec():
    return pl.BlockSpec((TI, C, N), lambda i, *_: (i, 0, 0))


def mask_spec_():
    return pl.BlockSpec((TI, N), lambda i, *_: (i, 0))


def piece_spec(k, n):
    return pl.BlockSpec((None, n, TI, N), lambda i: (k, 0, i, 0))


def half_spec():
    return pl.BlockSpec((H, TI, N), lambda i: (0, i, 0))


ACT = jax.ShapeDtypeStruct((RB, N, C), BF16)
ACTT = jax.ShapeDtypeStruct((RB, C, N), BF16)
HALF = jax.ShapeDtypeStruct((H, RB, N), BF16)
NPOS = RB * N


def cost(flops, nbytes, trans=0):
    return pl.CostEstimate(flops=int(flops), bytes_accessed=int(nbytes), transcendentals=int(trans))


def turn_body(z_ref, zt_ref):
    rows_loop(lambda i: put(zt_ref, i, jnp.concatenate([z_ref[G * i + r].T for r in range(G)], axis=1)), 1)


def turn(z):
    return pl.pallas_call(turn_body, grid=(RB // TI,), in_specs=[act_spec()], out_specs=actt_spec(), out_shape=ACTT,
                          cost_estimate=cost(NPOS * C * 40, NPOS * C * 4), name="turn")(z)


def norm_body(unroll, _, z_ref, ln_ref, *rest):
    zt_ref, xt_ref, xc_ref = rest[-3:]

    def row(i):
        zt = jnp.concatenate([z_ref[G * i + r].T for r in range(G)], axis=1)
        put(zt_ref, i, zt)
        h, _ = hat(zt.astype(F32))
        x = affine(h, ln_ref)
        put(xt_ref, i, x)
        put(xc_ref, i, x)

    rows_loop(row, unroll)


def norm(z, ln, part=0, full=None):
    rows = z.shape[0]
    extra = () if full is None else tuple(full)
    spec = pl.BlockSpec((TI, C, N), lambda i, p: (i + p[0], 0, 0))
    grid_spec = pltpu.PrefetchScalarGridSpec(
        num_scalar_prefetch=1, grid=(rows // TI,),
        in_specs=[act_spec(), const_spec((C, 2))] + [pl.BlockSpec(memory_space=pl.ANY)] * len(extra),
        out_specs=[spec, spec, actt_spec()])
    return pl.pallas_call(functools.partial(norm_body, 1), grid_spec=grid_spec, out_shape=[ACTT, ACTT, jax.ShapeDtypeStruct((rows, C, N), BF16)],
                          input_output_aliases={3: 0, 4: 1} if extra else {},
                          cost_estimate=cost(rows * N * C * 60, rows * N * C * 8), name="norm")(
        jnp.full((1,), part * (ZR // TI), jnp.int32), z, ln, *extra)


def prep_body(unroll, base, x_ref, m_ref, wt_ref, *rest):
    a_out, b_out, sa, sb = rest[-4:]

    def row(i):
        p = dot(wt_ref[...], get(x_ref, i) * get_mask(m_ref, i))
        for out, at in ((sa, 0), (sb, 2 * H)):
            lin = p[at:at + H]
            put(out, i, (lin * jnp.tanh(p[at + H:at + 2 * H]) + lin).astype(BF16))

    rows_loop(row, unroll)
    flush(sa, [a_out])
    flush(sb, [b_out])


def prep(base, xt, mask, wt, full=None, unroll=UNROLL):
    rows = xt.shape[0]
    npos = rows * N
    out = jax.ShapeDtypeStruct((H, N, N), BF16)
    spec = pl.BlockSpec((H, TI, N), lambda i, b: (0, b[0] + i, 0))
    extra = () if full is None else tuple(full)
    grid_spec = pltpu.PrefetchScalarGridSpec(
        num_scalar_prefetch=1, grid=(rows // TI,),
        in_specs=[actt_spec(), mask_spec_(), const_spec((4 * H, C))] + [pl.BlockSpec(memory_space=pl.ANY)] * len(extra),
        out_specs=[spec, spec], scratch_shapes=[scr(H), scr(H)])
    return pl.pallas_call(
        functools.partial(prep_body, unroll if rows == RB else 1), grid_spec=grid_spec, out_shape=[out, out],
        input_output_aliases={4: 0, 5: 1} if extra else {},
        cost_estimate=cost(npos * C * 400, npos * C * 4, npos * C), name="prep",
    )(base, xt, mask, wt, *extra)


def block_rows(idx, ref, c):
    return [ref[c, pl.ds(pl.multiple_of(idx[k] * RB, RB), RB), :] for k in range(4)]


def emit(vals, keep, send, c):
    keep[0, c] = vals[:RB]
    keep[1, c] = vals[RB:2 * RB]
    send[0, c] = vals[2 * RB:3 * RB]
    send[1, c] = vals[3 * RB:]


def tri_out_body(idx, a, b, keep, send):
    def chan(c):
        lhs = jnp.concatenate(block_rows(idx, a, c), axis=0)
        emit(dot(lhs, b[c], 1, 1).astype(BF16), keep, send, c)

    rows_loop(chan, 1, CB)


def tri_in_body(idx, a, b, keep, send, s):
    def chan(c):
        s[c] = a[c].T
        lhs = jnp.concatenate(block_rows(idx, s, c), axis=0)
        emit(dot(lhs, b[c]).astype(BF16), keep, send, c)

    rows_loop(chan, 1, CB)


def gather_dt(idx, parts, c, s):
    for k, part in enumerate(parts):
        s[c, pl.ds(pl.multiple_of(idx[k] * RB, RB), RB), :] = part[c]


def tri_in_bwd_body(idx, d0, d1, d2, d3, a, b, dak, das, dbk, dbs, s):
    def chan(c):
        gather_dt(idx, (d0, d1, d2, d3), c, s)
        emit(dot(jnp.concatenate(block_rows(idx, b, c), axis=0), s[c], 1, 1).astype(BF16), dak, das, c)
        emit(dot(jnp.concatenate(block_rows(idx, a, c), axis=0), s[c]).astype(BF16), dbk, dbs, c)

    rows_loop(chan, 1, CB)


def tri_out_bwd_body(idx, d0, d1, d2, d3, a, b, dak, das, dbk, dbs, s, st):
    def chan(c):
        gather_dt(idx, (d0, d1, d2, d3), c, s)
        da = dot(jnp.concatenate([d0[c], d2[c]], axis=0), b[c]).astype(BF16)
        st[c] = s[c].T
        rows = block_rows(idx, st, c)
        db = dot(jnp.concatenate([rows[0], rows[2]], axis=0), a[c]).astype(BF16)
        dak[0, c] = da[:RB]
        das[0, c] = da[RB:]
        dbk[0, c] = db[:RB]
        dbs[0, c] = db[RB:]

    rows_loop(chan, 1, CB)


def tri_call(body, idx, part, dts, ab, pieces, n_out, n_scr, flops):
    idx = jnp.concatenate([idx, jnp.full((1,), part * (HC // CB), jnp.int32)])
    dspec = pl.BlockSpec((CB, RB, N), lambda c, i: (c + i[4], 0, 0))
    fspec = pl.BlockSpec((CB, N, N), lambda c, i: (c + i[4], 0, 0))
    ospec = pl.BlockSpec((pieces, CB, RB, N), lambda c, _: (0, c, 0, 0))
    grid_spec = pltpu.PrefetchScalarGridSpec(
        num_scalar_prefetch=1, grid=(HC // CB,), in_specs=[dspec] * len(dts) + [fspec] * len(ab),
        out_specs=[ospec] * n_out, scratch_shapes=[pltpu.VMEM((CB, N, N), BF16)] * n_scr)
    return pl.pallas_call(body, grid_spec=grid_spec, out_shape=[jax.ShapeDtypeStruct((pieces, HC, RB, N), BF16)] * n_out,
                          cost_estimate=cost(flops, 50e6))(idx, *dts, *ab)


def finish_body(_, *refs):
    ts = refs[:2 * NCH]
    z_ref, x_ref, wg_ref, lnq_ref, wo_ref, ln_ref, z_out, x_out, st = refs[2 * NCH:]
    fill(st, ts)

    def row(i):
        th, _ = hat(get(st, i).astype(F32))
        upd = dot(wo_ref[...], affine(th, lnq_ref))
        gate = jnp.tanh(dot(wg_ref[...], get(x_ref, i)))
        zn = (get(z_ref, i).astype(F32) + (gate * upd + upd)).astype(BF16)
        put(z_out, i, zn)
        h, _ = hat(zn.astype(F32))
        put(x_out, i, affine(h, ln_ref))

    rows_loop(row)


def finish(k, ts, zt, xt, wgt, lnq, wot, ln_next):
    tspec = pl.BlockSpec((None, HC, TI, N), lambda i, p: (p[0], 0, i, 0))
    grid_spec = pltpu.PrefetchScalarGridSpec(
        num_scalar_prefetch=1, grid=(RB // TI,),
        in_specs=[tspec] * (2 * NCH) + [actt_spec(), actt_spec(), const_spec((C, C)), const_spec((C, 2)), const_spec((C, C)), const_spec((C, 2))],
        out_specs=[actt_spec()] * 2, scratch_shapes=[scr(C)])
    return pl.pallas_call(
        finish_body, grid_spec=grid_spec, out_shape=[ACTT] * 2,
        cost_estimate=cost(NPOS * C * 600, NPOS * C * 10, NPOS * C), name="finish",
    )(jnp.full((1,), k, jnp.int32), *ts, zt, xt, wgt, lnq, wot, ln_next)


def head_body(emit_z, emit_w, emit_dg, *refs):
    ts = refs[:2 * NCH]
    refs = list(refs[2 * NCH:])
    x_ref, g_ref, wg_ref, lnq_ref, wot_ref, wo_ref = refs[:6]
    k = 6
    if emit_z:
        z_ref = refs[k]
        k += 1
    dt_keep, dt_send = refs[k:k + 2]
    k += 2
    if emit_dg:
        dg_out = refs[k]
        k += 1
    if emit_z:
        z_out = refs[k]
        k += 1
    if emit_w:
        gwo, ggain, gshift = refs[k:k + 3]

        @pl.when(pl.program_id(0) == 0)
        def _():
            gwo[...] = jnp.zeros_like(gwo)
            ggain[...] = jnp.zeros_like(ggain)
            gshift[...] = jnp.zeros_like(gshift)

    st, sd = refs[-2:]
    fill(st, ts)

    def row(i):
        th, rstd = hat(get(st, i).astype(F32))
        if emit_dg:
            y = affine(th, lnq_ref)
            upd = dot(wot_ref[...], y)
        gate = jnp.tanh(dot(wg_ref[...], get(x_ref, i)))
        if emit_z:
            put_turned(z_out, i, (get(z_ref, i).astype(F32) + (gate * upd + upd)).astype(BF16))
        dgate = get(g_ref, i).astype(F32) * (0.5 * gate + 0.5)
        if emit_dg:
            put(dg_out, i, (dgate * (upd - upd * gate)).astype(BF16))
        du = dgate.astype(BF16)
        dy = dot(wo_ref[...], du).astype(BF16).astype(F32)
        dh = dy * lnq_ref[:, 0:1]
        m1 = jnp.sum(dh, axis=0, keepdims=True) * (1.0 / C)
        m2 = jnp.sum(dh * th, axis=0, keepdims=True) * (1.0 / C)
        put(sd, i, (rstd * (dh - m1 - th * m2)).astype(BF16))
        if emit_w:
            gwo[...] += dot(y, du, 1, 1)
            ggain[...] += fold(dy * th)
            gshift[...] += fold(dy)

    rows_loop(row)
    flush(sd, [dt_keep, dt_send])


def head(k, ts, xt, gt, wgt, lnq, wot, wo, zt=None, emit_w=False, emit_dg=True):
    emit_z = zt is not None
    in_specs = [piece_spec(k, HC)] * (2 * NCH) + [actt_spec(), actt_spec(), const_spec((C, C)), const_spec((C, 2)), const_spec((C, C)), const_spec((C, C))]
    out_shape = [HALF, HALF] + [ACTT] * emit_dg
    out_specs = [half_spec(), half_spec()] + [actt_spec()] * emit_dg
    extra = ()
    if emit_z:
        in_specs.append(actt_spec())
        extra = (zt,)
        out_shape.append(ACT)
        out_specs.append(act_spec())
    if emit_w:
        for s in ((C, C), (C, C), (C, C)):
            out_shape.append(jax.ShapeDtypeStruct(s, F32))
            out_specs.append(const_spec(s))
    return pl.pallas_call(
        functools.partial(head_body, emit_z, emit_w, emit_dg), grid=(RB // TI,), in_specs=in_specs,
        out_specs=out_specs, out_shape=out_shape, scratch_shapes=[scr(C), scr(C)],
        cost_estimate=cost(NPOS * C * 800, NPOS * C * 10, NPOS * C), name="head",
    )(*ts, xt, gt, wgt, lnq, wot, wo, *extra)


def back_body(n_ab, emit_w, last, *refs):
    das, dbs = refs[:n_ab], refs[n_ab:2 * n_ab]
    refs = refs[2 * n_ab:]
    z_ref, g_ref, dg_ref, m_ref, ln_ref, wt_ref, wb_ref, d_out = refs[:8]
    if emit_w:
        gw, ggain, gshift = refs[8:11]

        @pl.when(pl.program_id(0) == 0)
        def _():
            gw[...] = jnp.zeros_like(gw)
            ggain[...] = jnp.zeros_like(ggain)
            gshift[...] = jnp.zeros_like(gshift)

    sa, sb = refs[-2:]
    fill(sa, das)
    fill(sb, dbs)

    def row(i):
        xh, rstd = hat(get(z_ref, i).astype(F32))
        x = affine(xh, ln_ref)
        mrow = get_mask(m_ref, i)
        ds = []
        for s, at in ((sa, 0), (sb, 2 * C)):
            p = dot(wt_ref[at:at + 2 * C], x)
            th = jnp.tanh(p[C:])
            t0 = (get(s, i) * mrow).astype(F32) * (0.5 * th + 0.5)
            ds.append(t0.astype(BF16))
            ds.append((t0 * (p[:C] - p[:C] * th)).astype(BF16))
        dp = jnp.concatenate(ds + [get(dg_ref, i)], axis=0)
        dx = dot(wb_ref[...], dp).astype(BF16).astype(F32)
        dh = dx * ln_ref[:, 0:1]
        m1 = jnp.sum(dh, axis=0, keepdims=True) * (1.0 / C)
        m2 = jnp.sum(dh * xh, axis=0, keepdims=True) * (1.0 / C)
        d = (get(g_ref, i).astype(F32) + rstd * (dh - m1 - xh * m2)).astype(BF16)
        (put_turned if last else put)(d_out, i, d)
        if emit_w:
            gw[...] += dot(dp, x, 1, 1)
            ggain[...] += fold(dx * xh)
            gshift[...] += fold(dx)

    rows_loop(row, BACK_UNROLL if emit_w else UNROLL)


def back(k, das, dbs, zt, gt, dgt, mask, ln, wt, wb, emit_w, last):
    n = len(das)
    out_shape = [ACT if last else ACTT]
    out_specs = [act_spec() if last else actt_spec()]
    if emit_w:
        for s in ((5 * C, C), (C, C), (C, C)):
            out_shape.append(jax.ShapeDtypeStruct(s, F32))
            out_specs.append(const_spec(s))
    return pl.pallas_call(
        functools.partial(back_body, n, emit_w, last), grid=(RB // TI,),
        in_specs=[piece_spec(k, HC)] * (2 * n) + [actt_spec()] * 3 + [mask_spec_(), const_spec((C, 2)), const_spec((4 * C, C)), const_spec((C, 5 * C))],
        out_specs=out_specs, out_shape=out_shape, scratch_shapes=[scr(C), scr(C)],
        cost_estimate=cost(NPOS * C * 2000, NPOS * C * 12, NPOS * C * 2), name="back",
    )(*das, *dbs, zt, gt, dgt, mask, ln, wt, wb)


def solution(mesh):
    row_spec = P(('data', 'dap'), None, None)
    mask_spec = P(('data', 'dap'), None)
    full_spec = P()
    grad_spec = P('data', None, None)

    def ici(v):
        return lax.ppermute(v, AX, ICI_SWAP)

    def d2d(v):
        return lax.ppermute(v, AX, D2D_SWAP)

    def device_step(pair_act, pair_mask, d_pair_out, ln_pair, w_proj, w_gate, ln_chan, w_out):
        me = lax.axis_index(AX)
        odd = (me & 1) == 1
        blocks = jnp.stack([me ^ OWN, me ^ CROSS, me ^ PART, me ^ DIAG]).astype(jnp.int32)
        base = [blocks[k:k + 1] * (RB // TI) for k in range(4)]

        def local(v, axis):
            return jnp.where(odd, jnp.roll(v, H, axis=axis), v)

        m_own = pair_mask.astype(F32)
        m_cross = ici(m_own)
        m_part = d2d(m_own)
        m_diag = d2d(m_cross)

        ln = [ln_pair[u].T.astype(F32) for u in range(2)]
        lnq = [local(ln_chan[u].T.astype(F32), 0) for u in range(2)]
        wp4 = [local(w_proj[u].reshape(C, 4, C), 2) for u in range(2)]
        wt_half = [(0.5 * wp4[u][:, :, :H]).reshape(C, 4 * H).T for u in range(2)]
        wt = [(0.5 * wp4[u]).reshape(C, 4 * C).T for u in range(2)]
        wb = [jnp.concatenate([wp4[u].reshape(C, 4 * C), w_gate[u]], axis=1) for u in range(2)]
        wgt = [0.5 * w_gate[u].T for u in range(2)]
        wo = [local(w_out[u], 0) for u in range(2)]
        wot = [0.5 * wo[u].T for u in range(2)]

        def products(body, dts, a, b, pieces, n_scr, flops):
            n_out = 4 if dts else 2
            res, sent = [], []
            for part in range(NCH):
                res.append(tri_call(body, blocks, part, dts, (a, b), pieces, n_out, n_scr, flops / NCH))
                sent.append([d2d(res[-1][j]) for j in range(1, n_out, 2)])
            keeps = [[r[j] for r in res] for j in range(0, n_out, 2)]
            sends = [list(v) for v in zip(*sent)]
            return [k + s for k, s in zip(keeps, sends)]

        z_parts = []
        later = lax.optimization_barrier(pair_act)
        for j in range(ZC):
            z_parts.append(ici((later if j else pair_act)[j * ZR:(j + 1) * ZR]))
        zt_own, xt_own, _ = norm(pair_act, ln[0])
        xt_part = d2d(xt_own)
        gt_own = turn(d_pair_out)
        gt_cross = ici(gt_own)
        ab1 = prep(base[0], xt_own, m_own, wt_half[0], None, 1)
        ab1 = prep(base[2], xt_part, m_part, wt_half[0], ab1, 1)
        full = None
        for j in range(ZC):
            zt_cross, xt_cross, xc = norm(z_parts[j], ln[0], j, full)
            full = (zt_cross, xt_cross)
            xd = d2d(xc)
            rows = slice(j * ZR, (j + 1) * ZR)
            ab1 = prep(base[1] + j * (ZR // TI), xc, m_cross[rows], wt_half[0], ab1)
            ab1 = prep(base[3] + j * (ZR // TI), xd, m_diag[rows], wt_half[0], ab1)
        a1, b1 = ab1
        t1, = products(tri_out_body, (), a1, b1, 2, 0, 7.2e9)
        yt_own, vt_own = finish(0, t1, zt_own, xt_own, wgt[0], lnq[0], wot[0], ln[1])
        vt_part = d2d(vt_own)
        yt_cross, vt_cross = finish(1, t1, zt_cross, xt_cross, wgt[0], lnq[0], wot[0], ln[1])
        vt_diag = d2d(vt_cross)

        ab2 = prep(base[0], vt_own, m_own, wt_half[1])
        ab2 = prep(base[2], vt_part, m_part, wt_half[1], ab2)
        ab2 = prep(base[1], vt_cross, m_cross, wt_half[1], ab2)
        a2, b2 = prep(base[3], vt_diag, m_diag, wt_half[1], ab2)
        t2, = products(tri_in_body, (), a2, b2, 2, 1, 7.2e9)

        dk_own, ds_own, dg2_own, pair_out, gwo2, gq2g, gq2s = head(0, t2, vt_own, gt_own, wgt[1], lnq[1], wot[1], wo[1], yt_own, True)
        dk_part = d2d(ds_own)
        dk_cross, ds_cross, dg2_cross = head(1, t2, vt_cross, gt_cross, wgt[1], lnq[1], wot[1], wo[1])
        dk_diag = d2d(ds_cross)
        da2, db2 = products(tri_in_bwd_body, (dk_own, dk_cross, dk_part, dk_diag), a2, b2, 2, 1, 14.4e9)
        et_own, gw2, gp2g, gp2s = back(0, da2, db2, yt_own, gt_own, dg2_own, m_own, ln[1], wt[1], wb[1], True, False)
        et_cross, = back(1, da2, db2, yt_cross, gt_cross, dg2_cross, m_cross, ln[1], wt[1], wb[1], False, False)

        dk_own, ds_own, dg1_own, gwo1, gq1g, gq1s = head(0, t1, xt_own, et_own, wgt[0], lnq[0], wot[0], wo[0], None, True)
        dk_part = d2d(ds_own)

        def vec(gg, gs):
            return jnp.stack([jnp.sum(gg, axis=1), jnp.sum(gs, axis=1)])

        def common(g):
            return jnp.concatenate([local(g[:4 * C].reshape(4, C, C), 1).reshape(4 * C, C), g[4 * C:]], axis=0)

        def total(v):
            w = d2d(v)
            v = v + w
            w = ici(v)
            return v + w

        early = total(jnp.concatenate([common(gw2), local(gwo2, 0), local(gwo1, 0), vec(gp2g, gp2s),
                                       local(vec(gq2g, gq2s), 1), local(vec(gq1g, gq1s), 1), jnp.zeros((2, C), F32)], axis=0))
        dk_cross, ds_cross = head(1, t1, xt_cross, et_cross, wgt[0], lnq[0], wot[0], wo[0], None, False, False)
        dk_diag = d2d(ds_cross)
        da1, db1 = products(tri_out_bwd_body, (dk_own, dk_cross, dk_part, dk_diag), a1, b1, 1, 2, 7.2e9)
        d_pair, gw1, gp1g, gp1s = back(0, da1, db1, zt_own, et_own, dg1_own, m_own, ln[0], wt[0], wb[0], True, True)
        late = total(jnp.concatenate([common(gw1), vec(gp1g, gp1s), jnp.zeros((6, C), F32)], axis=0))
        e0, e1, e2 = 5 * C, 6 * C, 7 * C
        grads = (jnp.stack([late[e0:e0 + 2], early[e2:e2 + 2]]),
                 jnp.stack([late[:4 * C].T, early[:4 * C].T]),
                 jnp.stack([late[4 * C:e0].T, early[4 * C:e0].T]),
                 jnp.stack([early[e2 + 4:e2 + 6], early[e2 + 2:e2 + 4]]),
                 jnp.stack([early[e1:e2], early[e0:e1]]))
        return (pair_out, d_pair) + tuple(v.astype(BF16) for v in grads)


    return jax.shard_map(device_step, mesh=mesh, in_specs=(row_spec, mask_spec, row_spec, full_spec, full_spec, full_spec, full_spec, full_spec), out_specs=(row_spec, row_spec, grad_spec, grad_spec, grad_spec, grad_spec, grad_spec), check_vma=False)
```

```python
import functools
import jax
import jax.numpy as jnp
from jax import lax
from jax.experimental import pallas as pl
from jax.experimental.pallas import tpu as pltpu
from jax.sharding import PartitionSpec as P

LN_EPS = 1e-5
AX = 'dap'
N = 384
C = 128
H = 64
TI = 16
RB = 96
CB = 8
NCH = 2
HC = H // NCH
UNROLL = 2
G = 2
ZC = 6
BACK_UNROLL = 4
ZR = RB // ZC
F32 = jnp.float32
BF16 = jnp.bfloat16
ICI_SWAP = [(0, 2), (2, 0), (1, 3), (3, 1)]
D2D_SWAP = [(0, 1), (1, 0), (2, 3), (3, 2)]
OWN, CROSS, PART, DIAG = 0, 2, 1, 3


def dot(a, b, ca=1, cb=0):
    return lax.dot_general(a, b, (((ca,), (cb,)), ((), ())), preferred_element_type=F32)


def hat(v):
    mean = jnp.sum(v, axis=0, keepdims=True) * (1.0 / C)
    cen = v - mean
    var = jnp.sum(cen * cen, axis=0, keepdims=True) * (1.0 / C)
    rstd = lax.rsqrt(var + LN_EPS)
    return cen * rstd, rstd


def affine(h, ln_ref):
    return (h * ln_ref[:, 0:1] + ln_ref[:, 1:2]).astype(BF16)


def rows_loop(fn, unroll=UNROLL, n=TI // G):
    def step(i, carry):
        fn(i)
        return carry

    lax.fori_loop(0, n, step, 0, unroll=unroll)


def get(ref, i):
    return jnp.concatenate([ref[G * i + r] for r in range(G)], axis=1)


def put(ref, i, v):
    for r in range(G):
        ref[G * i + r] = v[:, r * N:(r + 1) * N]


def put_turned(ref, i, v):
    for r in range(G):
        ref[G * i + r] = v[:, r * N:(r + 1) * N].T


def get_mask(ref, i):
    return jnp.concatenate([ref[pl.ds(G * i + r, 1), :] for r in range(G)], axis=1).astype(BF16)


def fold(v):
    return functools.reduce(lambda p, q: p + q, [v[:, k * 128:(k + 1) * 128] for k in range(G * N // 128)])


def fill(scr, refs):
    at = 0
    for ref in refs:
        def move(k, ref=ref, at=at):
            c = pl.multiple_of(k * 16, 16)
            scr[:, pl.ds(at + c, 16), :] = jnp.swapaxes(ref[pl.ds(c, 16)], 0, 1)

        rows_loop(move, 1, ref.shape[0] // 16)
        at += ref.shape[0]


def flush(scr, refs):
    at = 0
    for ref in refs:
        def move(k, ref=ref, at=at):
            c = pl.multiple_of(k * 16, 16)
            ref[pl.ds(c, 16)] = jnp.swapaxes(scr[:, pl.ds(at + c, 16), :], 0, 1)

        rows_loop(move, 1, ref.shape[0] // 16)
        at += ref.shape[0]


def scr(n):
    return pltpu.VMEM((TI, n, N), BF16)


def const_spec(shape):
    nd = len(shape)
    return pl.BlockSpec(shape, lambda *_: (0,) * nd)


def act_spec():
    return pl.BlockSpec((TI, N, C), lambda i, *_: (i, 0, 0))


def actt_spec():
    return pl.BlockSpec((TI, C, N), lambda i, *_: (i, 0, 0))


def mask_spec_():
    return pl.BlockSpec((TI, N), lambda i, *_: (i, 0))


def piece_spec(k, n):
    return pl.BlockSpec((None, n, TI, N), lambda i: (k, 0, i, 0))


def half_spec():
    return pl.BlockSpec((H, TI, N), lambda i: (0, i, 0))


ACT = jax.ShapeDtypeStruct((RB, N, C), BF16)
ACTT = jax.ShapeDtypeStruct((RB, C, N), BF16)
HALF = jax.ShapeDtypeStruct((H, RB, N), BF16)
NPOS = RB * N


def cost(flops, nbytes, trans=0):
    return pl.CostEstimate(flops=int(flops), bytes_accessed=int(nbytes), transcendentals=int(trans))


def turn_body(z_ref, zt_ref):
    rows_loop(lambda i: put(zt_ref, i, jnp.concatenate([z_ref[G * i + r].T for r in range(G)], axis=1)), 1)


def turn(z):
    return pl.pallas_call(turn_body, grid=(RB // TI,), in_specs=[act_spec()], out_specs=actt_spec(), out_shape=ACTT,
                          cost_estimate=cost(NPOS * C * 40, NPOS * C * 4), name="turn")(z)


def norm_body(unroll, _, z_ref, ln_ref, *rest):
    zt_ref, xt_ref, xc_ref = rest[-3:]

    def row(i):
        zt = jnp.concatenate([z_ref[G * i + r].T for r in range(G)], axis=1)
        put(zt_ref, i, zt)
        h, _ = hat(zt.astype(F32))
        x = affine(h, ln_ref)
        put(xt_ref, i, x)
        put(xc_ref, i, x)

    rows_loop(row, unroll)


def norm(z, ln, part=0, full=None):
    rows = z.shape[0]
    extra = () if full is None else tuple(full)
    spec = pl.BlockSpec((TI, C, N), lambda i, p: (i + p[0], 0, 0))
    grid_spec = pltpu.PrefetchScalarGridSpec(
        num_scalar_prefetch=1, grid=(rows // TI,),
        in_specs=[act_spec(), const_spec((C, 2))] + [pl.BlockSpec(memory_space=pl.ANY)] * len(extra),
        out_specs=[spec, spec, actt_spec()])
    return pl.pallas_call(functools.partial(norm_body, 1), grid_spec=grid_spec, out_shape=[ACTT, ACTT, jax.ShapeDtypeStruct((rows, C, N), BF16)],
                          input_output_aliases={3: 0, 4: 1} if extra else {},
                          cost_estimate=cost(rows * N * C * 60, rows * N * C * 8), name="norm")(
        jnp.full((1,), part * (ZR // TI), jnp.int32), z, ln, *extra)


def prep_body(unroll, base, x_ref, m_ref, wt_ref, *rest):
    a_out, b_out, sa, sb = rest[-4:]

    def row(i):
        p = dot(wt_ref[...], get(x_ref, i) * get_mask(m_ref, i))
        for out, at in ((sa, 0), (sb, 2 * H)):
            lin = p[at:at + H]
            put(out, i, (lin * jnp.tanh(p[at + H:at + 2 * H]) + lin).astype(BF16))

    rows_loop(row, unroll)
    flush(sa, [a_out])
    flush(sb, [b_out])


def prep(base, xt, mask, wt, full=None, unroll=UNROLL):
    rows = xt.shape[0]
    npos = rows * N
    out = jax.ShapeDtypeStruct((H, N, N), BF16)
    spec = pl.BlockSpec((H, TI, N), lambda i, b: (0, b[0] + i, 0))
    extra = () if full is None else tuple(full)
    grid_spec = pltpu.PrefetchScalarGridSpec(
        num_scalar_prefetch=1, grid=(rows // TI,),
        in_specs=[actt_spec(), mask_spec_(), const_spec((4 * H, C))] + [pl.BlockSpec(memory_space=pl.ANY)] * len(extra),
        out_specs=[spec, spec], scratch_shapes=[scr(H), scr(H)])
    return pl.pallas_call(
        functools.partial(prep_body, unroll if rows == RB else 1), grid_spec=grid_spec, out_shape=[out, out],
        input_output_aliases={4: 0, 5: 1} if extra else {},
        cost_estimate=cost(npos * C * 400, npos * C * 4, npos * C), name="prep",
    )(base, xt, mask, wt, *extra)


def block_rows(idx, ref, c):
    return [ref[c, pl.ds(pl.multiple_of(idx[k] * RB, RB), RB), :] for k in range(4)]


def emit(vals, keep, send, c):
    keep[0, c] = vals[:RB]
    keep[1, c] = vals[RB:2 * RB]
    send[0, c] = vals[2 * RB:3 * RB]
    send[1, c] = vals[3 * RB:]


def tri_out_body(idx, a, b, keep, send):
    def chan(c):
        lhs = jnp.concatenate(block_rows(idx, a, c), axis=0)
        emit(dot(lhs, b[c], 1, 1).astype(BF16), keep, send, c)

    rows_loop(chan, 2, CB)


def tri_in_body(idx, a, b, keep, send, s):
    def chan(c):
        s[c] = a[c].T
        lhs = jnp.concatenate(block_rows(idx, s, c), axis=0)
        emit(dot(lhs, b[c]).astype(BF16), keep, send, c)

    rows_loop(chan, 2, CB)


def gather_dt(idx, parts, c, s):
    for k, part in enumerate(parts):
        s[c, pl.ds(pl.multiple_of(idx[k] * RB, RB), RB), :] = part[c]


def tri_in_bwd_body(idx, d0, d1, d2, d3, a, b, dak, das, dbk, dbs, s):
    def chan(c):
        gather_dt(idx, (d0, d1, d2, d3), c, s)
        emit(dot(jnp.concatenate(block_rows(idx, b, c), axis=0), s[c], 1, 1).astype(BF16), dak, das, c)
        emit(dot(jnp.concatenate(block_rows(idx, a, c), axis=0), s[c]).astype(BF16), dbk, dbs, c)

    rows_loop(chan, 1, CB)


def tri_out_bwd_body(idx, d0, d1, d2, d3, a, b, dak, das, dbk, dbs, s, st):
    def chan(c):
        gather_dt(idx, (d0, d1, d2, d3), c, s)
        da = dot(jnp.concatenate([d0[c], d2[c]], axis=0), b[c]).astype(BF16)
        st[c] = s[c].T
        rows = block_rows(idx, st, c)
        db = dot(jnp.concatenate([rows[0], rows[2]], axis=0), a[c]).astype(BF16)
        dak[0, c] = da[:RB]
        das[0, c] = da[RB:]
        dbk[0, c] = db[:RB]
        dbs[0, c] = db[RB:]

    rows_loop(chan, 2, CB)


def tri_call(body, idx, part, dts, ab, pieces, n_out, n_scr, flops):
    idx = jnp.concatenate([idx, jnp.full((1,), part * (HC // CB), jnp.int32)])
    dspec = pl.BlockSpec((CB, RB, N), lambda c, i: (c + i[4], 0, 0))
    fspec = pl.BlockSpec((CB, N, N), lambda c, i: (c + i[4], 0, 0))
    ospec = pl.BlockSpec((pieces, CB, RB, N), lambda c, _: (0, c, 0, 0))
    grid_spec = pltpu.PrefetchScalarGridSpec(
        num_scalar_prefetch=1, grid=(HC // CB,), in_specs=[dspec] * len(dts) + [fspec] * len(ab),
        out_specs=[ospec] * n_out, scratch_shapes=[pltpu.VMEM((CB, N, N), BF16)] * n_scr)
    return pl.pallas_call(body, grid_spec=grid_spec, out_shape=[jax.ShapeDtypeStruct((pieces, HC, RB, N), BF16)] * n_out,
                          cost_estimate=cost(flops, 50e6))(idx, *dts, *ab)


def finish_body(_, *refs):
    ts = refs[:2 * NCH]
    z_ref, x_ref, wg_ref, lnq_ref, wo_ref, ln_ref, z_out, x_out, st = refs[2 * NCH:]
    fill(st, ts)

    def row(i):
        th, _ = hat(get(st, i).astype(F32))
        upd = dot(wo_ref[...], affine(th, lnq_ref))
        gate = jnp.tanh(dot(wg_ref[...], get(x_ref, i)))
        zn = (get(z_ref, i).astype(F32) + (gate * upd + upd)).astype(BF16)
        put(z_out, i, zn)
        h, _ = hat(zn.astype(F32))
        put(x_out, i, affine(h, ln_ref))

    rows_loop(row)


def finish(k, ts, zt, xt, wgt, lnq, wot, ln_next):
    tspec = pl.BlockSpec((None, HC, TI, N), lambda i, p: (p[0], 0, i, 0))
    grid_spec = pltpu.PrefetchScalarGridSpec(
        num_scalar_prefetch=1, grid=(RB // TI,),
        in_specs=[tspec] * (2 * NCH) + [actt_spec(), actt_spec(), const_spec((C, C)), const_spec((C, 2)), const_spec((C, C)), const_spec((C, 2))],
        out_specs=[actt_spec()] * 2, scratch_shapes=[scr(C)])
    return pl.pallas_call(
        finish_body, grid_spec=grid_spec, out_shape=[ACTT] * 2,
        cost_estimate=cost(NPOS * C * 600, NPOS * C * 10, NPOS * C), name="finish",
    )(jnp.full((1,), k, jnp.int32), *ts, zt, xt, wgt, lnq, wot, ln_next)


def head_body(emit_z, emit_w, emit_dg, *refs):
    ts = refs[:2 * NCH]
    refs = list(refs[2 * NCH:])
    x_ref, g_ref, wg_ref, lnq_ref, wot_ref, wo_ref = refs[:6]
    k = 6
    if emit_z:
        z_ref = refs[k]
        k += 1
    dt_keep, dt_send = refs[k:k + 2]
    k += 2
    if emit_dg:
        dg_out = refs[k]
        k += 1
    if emit_z:
        z_out = refs[k]
        k += 1
    if emit_w:
        gwo, ggain, gshift = refs[k:k + 3]

        @pl.when(pl.program_id(0) == 0)
        def _():
            gwo[...] = jnp.zeros_like(gwo)
            ggain[...] = jnp.zeros_like(ggain)
            gshift[...] = jnp.zeros_like(gshift)

    st, sd = refs[-2:]
    fill(st, ts)

    def row(i):
        th, rstd = hat(get(st, i).astype(F32))
        if emit_dg:
            y = affine(th, lnq_ref)
            upd = dot(wot_ref[...], y)
        gate = jnp.tanh(dot(wg_ref[...], get(x_ref, i)))
        if emit_z:
            put_turned(z_out, i, (get(z_ref, i).astype(F32) + (gate * upd + upd)).astype(BF16))
        dgate = get(g_ref, i).astype(F32) * (0.5 * gate + 0.5)
        if emit_dg:
            put(dg_out, i, (dgate * (upd - upd * gate)).astype(BF16))
        du = dgate.astype(BF16)
        dy = dot(wo_ref[...], du).astype(BF16).astype(F32)
        dh = dy * lnq_ref[:, 0:1]
        m1 = jnp.sum(dh, axis=0, keepdims=True) * (1.0 / C)
        m2 = jnp.sum(dh * th, axis=0, keepdims=True) * (1.0 / C)
        put(sd, i, (rstd * (dh - m1 - th * m2)).astype(BF16))
        if emit_w:
            gwo[...] += dot(y, du, 1, 1)
            ggain[...] += fold(dy * th)
            gshift[...] += fold(dy)

    rows_loop(row, UNROLL if emit_dg else 1)
    flush(sd, [dt_keep, dt_send])


def head(k, ts, xt, gt, wgt, lnq, wot, wo, zt=None, emit_w=False, emit_dg=True):
    emit_z = zt is not None
    in_specs = [piece_spec(k, HC)] * (2 * NCH) + [actt_spec(), actt_spec(), const_spec((C, C)), const_spec((C, 2)), const_spec((C, C)), const_spec((C, C))]
    out_shape = [HALF, HALF] + [ACTT] * emit_dg
    out_specs = [half_spec(), half_spec()] + [actt_spec()] * emit_dg
    extra = ()
    if emit_z:
        in_specs.append(actt_spec())
        extra = (zt,)
        out_shape.append(ACT)
        out_specs.append(act_spec())
    if emit_w:
        for s in ((C, C), (C, C), (C, C)):
            out_shape.append(jax.ShapeDtypeStruct(s, F32))
            out_specs.append(const_spec(s))
    return pl.pallas_call(
        functools.partial(head_body, emit_z, emit_w, emit_dg), grid=(RB // TI,), in_specs=in_specs,
        out_specs=out_specs, out_shape=out_shape, scratch_shapes=[scr(C), scr(C)],
        cost_estimate=cost(NPOS * C * 800, NPOS * C * 10, NPOS * C), name="head",
    )(*ts, xt, gt, wgt, lnq, wot, wo, *extra)


def back_body(n_ab, emit_w, last, *refs):
    das, dbs = refs[:n_ab], refs[n_ab:2 * n_ab]
    refs = refs[2 * n_ab:]
    z_ref, g_ref, dg_ref, m_ref, ln_ref, wt_ref, wb_ref, d_out = refs[:8]
    if emit_w:
        gw, ggain, gshift = refs[8:11]

        @pl.when(pl.program_id(0) == 0)
        def _():
            gw[...] = jnp.zeros_like(gw)
            ggain[...] = jnp.zeros_like(ggain)
            gshift[...] = jnp.zeros_like(gshift)

    sa, sb = refs[-2:]
    fill(sa, das)
    fill(sb, dbs)

    def row(i):
        xh, rstd = hat(get(z_ref, i).astype(F32))
        x = affine(xh, ln_ref)
        mrow = get_mask(m_ref, i)
        ds = []
        for s, at in ((sa, 0), (sb, 2 * C)):
            p = dot(wt_ref[at:at + 2 * C], x)
            th = jnp.tanh(p[C:])
            t0 = (get(s, i) * mrow).astype(F32) * (0.5 * th + 0.5)
            ds.append(t0.astype(BF16))
            ds.append((t0 * (p[:C] - p[:C] * th)).astype(BF16))
        dp = jnp.concatenate(ds + [get(dg_ref, i)], axis=0)
        dx = dot(wb_ref[...], dp).astype(BF16).astype(F32)
        dh = dx * ln_ref[:, 0:1]
        m1 = jnp.sum(dh, axis=0, keepdims=True) * (1.0 / C)
        m2 = jnp.sum(dh * xh, axis=0, keepdims=True) * (1.0 / C)
        d = (get(g_ref, i).astype(F32) + rstd * (dh - m1 - xh * m2)).astype(BF16)
        (put_turned if last else put)(d_out, i, d)
        if emit_w:
            gw[...] += dot(dp, x, 1, 1)
            ggain[...] += fold(dx * xh)
            gshift[...] += fold(dx)

    rows_loop(row, BACK_UNROLL if emit_w else UNROLL)


def back(k, das, dbs, zt, gt, dgt, mask, ln, wt, wb, emit_w, last):
    n = len(das)
    out_shape = [ACT if last else ACTT]
    out_specs = [act_spec() if last else actt_spec()]
    if emit_w:
        for s in ((5 * C, C), (C, C), (C, C)):
            out_shape.append(jax.ShapeDtypeStruct(s, F32))
            out_specs.append(const_spec(s))
    return pl.pallas_call(
        functools.partial(back_body, n, emit_w, last), grid=(RB // TI,),
        in_specs=[piece_spec(k, HC)] * (2 * n) + [actt_spec()] * 3 + [mask_spec_(), const_spec((C, 2)), const_spec((4 * C, C)), const_spec((C, 5 * C))],
        out_specs=out_specs, out_shape=out_shape, scratch_shapes=[scr(C), scr(C)],
        cost_estimate=cost(NPOS * C * 2000, NPOS * C * 12, NPOS * C * 2), name="back",
    )(*das, *dbs, zt, gt, dgt, mask, ln, wt, wb)


def solution(mesh):
    row_spec = P(('data', 'dap'), None, None)
    mask_spec = P(('data', 'dap'), None)
    full_spec = P()
    grad_spec = P('data', None, None)

    def ici(v):
        return lax.ppermute(v, AX, ICI_SWAP)

    def d2d(v):
        return lax.ppermute(v, AX, D2D_SWAP)

    def device_step(pair_act, pair_mask, d_pair_out, ln_pair, w_proj, w_gate, ln_chan, w_out):
        me = lax.axis_index(AX)
        odd = (me & 1) == 1
        blocks = jnp.stack([me ^ OWN, me ^ CROSS, me ^ PART, me ^ DIAG]).astype(jnp.int32)
        base = [blocks[k:k + 1] * (RB // TI) for k in range(4)]

        def local(v, axis):
            return jnp.where(odd, jnp.roll(v, H, axis=axis), v)

        m_own = pair_mask.astype(F32)
        m_cross = ici(m_own)
        m_part = d2d(m_own)
        m_diag = d2d(m_cross)

        ln = [ln_pair[u].T.astype(F32) for u in range(2)]
        lnq = [local(ln_chan[u].T.astype(F32), 0) for u in range(2)]
        wp4 = [local(w_proj[u].reshape(C, 4, C), 2) for u in range(2)]
        wt_half = [(0.5 * wp4[u][:, :, :H]).reshape(C, 4 * H).T for u in range(2)]
        wt = [(0.5 * wp4[u]).reshape(C, 4 * C).T for u in range(2)]
        wb = [jnp.concatenate([wp4[u].reshape(C, 4 * C), w_gate[u]], axis=1) for u in range(2)]
        wgt = [0.5 * w_gate[u].T for u in range(2)]
        wo = [local(w_out[u], 0) for u in range(2)]
        wot = [0.5 * wo[u].T for u in range(2)]

        def products(body, dts, a, b, pieces, n_scr, flops):
            n_out = 4 if dts else 2
            res, sent = [], []
            for part in range(NCH):
                res.append(tri_call(body, blocks, part, dts, (a, b), pieces, n_out, n_scr, flops / NCH))
                sent.append([d2d(res[-1][j]) for j in range(1, n_out, 2)])
            keeps = [[r[j] for r in res] for j in range(0, n_out, 2)]
            sends = [list(v) for v in zip(*sent)]
            return [k + s for k, s in zip(keeps, sends)]

        z_parts = []
        later = lax.optimization_barrier(pair_act)
        for j in range(ZC):
            z_parts.append(ici((later if j else pair_act)[j * ZR:(j + 1) * ZR]))
        zt_own, xt_own, _ = norm(pair_act, ln[0])
        xt_part = d2d(xt_own)
        gt_own = turn(d_pair_out)
        gt_cross = ici(gt_own)
        ab1 = prep(base[0], xt_own, m_own, wt_half[0], None, 1)
        ab1 = prep(base[2], xt_part, m_part, wt_half[0], ab1, 1)
        full = None
        for j in range(ZC):
            zt_cross, xt_cross, xc = norm(z_parts[j], ln[0], j, full)
            full = (zt_cross, xt_cross)
            xd = d2d(xc)
            rows = slice(j * ZR, (j + 1) * ZR)
            ab1 = prep(base[1] + j * (ZR // TI), xc, m_cross[rows], wt_half[0], ab1)
            ab1 = prep(base[3] + j * (ZR // TI), xd, m_diag[rows], wt_half[0], ab1)
        a1, b1 = ab1
        t1, = products(tri_out_body, (), a1, b1, 2, 0, 7.2e9)
        yt_own, vt_own = finish(0, t1, zt_own, xt_own, wgt[0], lnq[0], wot[0], ln[1])
        vt_part = d2d(vt_own)
        yt_cross, vt_cross = finish(1, t1, zt_cross, xt_cross, wgt[0], lnq[0], wot[0], ln[1])
        vt_diag = d2d(vt_cross)

        ab2 = prep(base[0], vt_own, m_own, wt_half[1])
        ab2 = prep(base[2], vt_part, m_part, wt_half[1], ab2)
        ab2 = prep(base[1], vt_cross, m_cross, wt_half[1], ab2)
        a2, b2 = prep(base[3], vt_diag, m_diag, wt_half[1], ab2)
        t2, = products(tri_in_body, (), a2, b2, 2, 1, 7.2e9)

        dk_own, ds_own, dg2_own, pair_out, gwo2, gq2g, gq2s = head(0, t2, vt_own, gt_own, wgt[1], lnq[1], wot[1], wo[1], yt_own, True)
        dk_part = d2d(ds_own)
        dk_cross, ds_cross, dg2_cross = head(1, t2, vt_cross, gt_cross, wgt[1], lnq[1], wot[1], wo[1])
        dk_diag = d2d(ds_cross)
        da2, db2 = products(tri_in_bwd_body, (dk_own, dk_cross, dk_part, dk_diag), a2, b2, 2, 1, 14.4e9)
        et_own, gw2, gp2g, gp2s = back(0, da2, db2, yt_own, gt_own, dg2_own, m_own, ln[1], wt[1], wb[1], True, False)
        et_cross, = back(1, da2, db2, yt_cross, gt_cross, dg2_cross, m_cross, ln[1], wt[1], wb[1], False, False)

        dk_own, ds_own, dg1_own, gwo1, gq1g, gq1s = head(0, t1, xt_own, et_own, wgt[0], lnq[0], wot[0], wo[0], None, True)
        dk_part = d2d(ds_own)

        def vec(gg, gs):
            return jnp.stack([jnp.sum(gg, axis=1), jnp.sum(gs, axis=1)])

        def common(g):
            return jnp.concatenate([local(g[:4 * C].reshape(4, C, C), 1).reshape(4 * C, C), g[4 * C:]], axis=0)

        def total(v):
            w = d2d(v)
            v = v + w
            w = ici(v)
            return v + w

        early = total(jnp.concatenate([common(gw2), local(gwo2, 0), local(gwo1, 0), vec(gp2g, gp2s),
                                       local(vec(gq2g, gq2s), 1), local(vec(gq1g, gq1s), 1), jnp.zeros((2, C), F32)], axis=0))
        dk_cross, ds_cross = head(1, t1, xt_cross, et_cross, wgt[0], lnq[0], wot[0], wo[0], None, False, False)
        dk_diag = d2d(ds_cross)
        da1, db1 = products(tri_out_bwd_body, (dk_own, dk_cross, dk_part, dk_diag), a1, b1, 1, 2, 7.2e9)
        d_pair, gw1, gp1g, gp1s = back(0, da1, db1, zt_own, et_own, dg1_own, m_own, ln[0], wt[0], wb[0], True, True)
        late = total(jnp.concatenate([common(gw1), vec(gp1g, gp1s), jnp.zeros((6, C), F32)], axis=0))
        e0, e1, e2 = 5 * C, 6 * C, 7 * C
        grads = (jnp.stack([late[e0:e0 + 2], early[e2:e2 + 2]]),
                 jnp.stack([late[:4 * C].T, early[:4 * C].T]),
                 jnp.stack([late[4 * C:e0].T, early[4 * C:e0].T]),
                 jnp.stack([early[e2 + 4:e2 + 6], early[e2 + 2:e2 + 4]]),
                 jnp.stack([early[e1:e2], early[e0:e1]]))
        return (pair_out, d_pair) + tuple(v.astype(BF16) for v in grads)


    return jax.shard_map(device_step, mesh=mesh, in_specs=(row_spec, mask_spec, row_spec, full_spec, full_spec, full_spec, full_spec, full_spec), out_specs=(row_spec, row_spec, grad_spec, grad_spec, grad_spec, grad_spec, grad_spec), check_vma=False)
```
